32 devices in a mesh: layer: 2 (over x), tp: 4 (over z), fsdp: 4 (over y, core).
Axes of the slice: x: 2, y: 2, z: 4, core: 2. Of those that a mesh axis runs over, the one named last changes fastest.
Arguments:
- wq_weight: float32 [4096, 2048], P(('layer', 'fsdp'), 'tp'), parts along dimension 0
- wq_moment: float32 [4096, 2048], P(('layer', 'fsdp'), 'tp'), parts along dimension 0
- wq_grad: bfloat16 [4096, 2048], P(('layer', 'fsdp'), 'tp'), parts along dimension 0
- wq_factor: float32 [4096, 128], P(('layer', 'tp')), parts along dimension 0
- wk_weight: float32 [4096, 2048], P(('layer', 'fsdp'), 'tp'), parts along dimension 0
- wk_moment: float32 [4096, 2048], P(('layer', 'fsdp'), 'tp'), parts along dimension 0
- wk_grad: bfloat16 [4096, 2048], P(('layer', 'fsdp'), 'tp'), parts along dimension 0
- wk_factor: float32 [4096, 128], P(('layer', 'tp')), parts along dimension 0
- wv_weight: float32 [4096, 2048], P(('layer', 'fsdp'), 'tp'), parts along dimension 0
- wv_moment: float32 [4096, 2048], P(('layer', 'fsdp'), 'tp'), parts along dimension 0
- wv_grad: bfloat16 [4096, 2048], P(('layer', 'fsdp'), 'tp'), parts along dimension 0
- wv_factor: float32 [4096, 128], P(('layer', 'tp')), parts along dimension 0
- wo_weight: float32 [4096, 2048], P(('layer', 'fsdp'), 'tp'), parts along dimension 0
- wo_moment: float32 [4096, 2048], P(('layer', 'fsdp'), 'tp'), parts along dimension 0
- wo_grad: bfloat16 [4096, 2048], P(('layer', 'fsdp'), 'tp'), parts along dimension 0
- wo_factor: float32 [4096, 128], P(('layer', 'tp')), parts along dimension 0
- gate_weight: float32 [6, 2048, 1408], P('layer', 'fsdp', 'tp'), parts along dimension 0
- gate_moment: float32 [6, 2048, 1408], P('layer', 'fsdp', 'tp'), parts along dimension 0
- gate_grad: bfloat16 [6, 2048, 1408], P('layer', 'fsdp', 'tp'), parts along dimension 0
- gate_factor: float32 [6, 1408, 88], P('layer', 'tp'), parts along dimension 0
- up_weight: float32 [6, 2048, 1408], P('layer', 'fsdp', 'tp'), parts along dimension 0
- up_moment: float32 [6, 2048, 1408], P('layer', 'fsdp', 'tp'), parts along dimension 0
- up_grad: bfloat16 [6, 2048, 1408], P('layer', 'fsdp', 'tp'), parts along dimension 0
- up_factor: float32 [6, 1408, 88], P('layer', 'tp'), parts along dimension 0
- down_weight: float32 [6, 1408, 2048], P('layer', 'fsdp', 'tp'), parts along dimension 0
- down_moment: float32 [6, 1408, 2048], P('layer', 'fsdp', 'tp'), parts along dimension 0
- down_grad: bfloat16 [6, 1408, 2048], P('layer', 'fsdp', 'tp'), parts along dimension 0
- down_factor: float32 [6, 1408, 88], P('layer', 'fsdp'), parts along dimension 0
Outputs:
- output 1: float32 [4096, 2048], P(('layer', 'fsdp'), 'tp'), parts along dimension 0
- output 2: float32 [4096, 2048], P(('layer', 'fsdp'), 'tp'), parts along dimension 0
- output 3: float32 [4096, 128], P(('layer', 'tp')), parts along dimension 0
- output 4: float32 [4096, 2048], P(('layer', 'fsdp'), 'tp'), parts along dimension 0
- output 5: float32 [4096, 2048], P(('layer', 'fsdp'), 'tp'), parts along dimension 0
- output 6: float32 [4096, 128], P(('layer', 'tp')), parts along dimension 0
- output 7: float32 [4096, 2048], P(('layer', 'fsdp'), 'tp'), parts along dimension 0
- output 8: float32 [4096, 2048], P(('layer', 'fsdp'), 'tp'), parts along dimension 0
- output 9: float32 [4096, 128], P(('layer', 'tp')), parts along dimension 0
- output 10: float32 [4096, 2048], P(('layer', 'fsdp'), 'tp'), parts along dimension 0
- output 11: float32 [4096, 2048], P(('layer', 'fsdp'), 'tp'), parts along dimension 0
- output 12: float32 [4096, 128], P(('layer', 'tp')), parts along dimension 0
- output 13: float32 [6, 2048, 1408], P('layer', 'fsdp', 'tp'), parts along dimension 0
- output 14: float32 [6, 2048, 1408], P('layer', 'fsdp', 'tp'), parts along dimension 0
- output 15: float32 [6, 1408, 88], P('layer', 'tp'), parts along dimension 0
- output 16: float32 [6, 2048, 1408], P('layer', 'fsdp', 'tp'), parts along dimension 0
- output 17: float32 [6, 2048, 1408], P('layer', 'fsdp', 'tp'), parts along dimension 0
- output 18: float32 [6, 1408, 88], P('layer', 'tp'), parts along dimension 0
- output 19: float32 [6, 1408, 2048], P('layer', 'fsdp', 'tp'), parts along dimension 0
- output 20: float32 [6, 1408, 2048], P('layer', 'fsdp', 'tp'), parts along dimension 0
- output 21: float32 [6, 1408, 88], P('layer', 'fsdp'), parts along dimension 0
There are 2 independent parts. The reference program is written for one: setup_inputs(seed, part) draws one part's arguments, and reference() takes and returns one part's arrays. A program takes and returns all parts, laid end to end along the dimension named above; each array names one.
All inputs are finite; a program needn't handle non-finite values.
Results may differ from the reference program's by a relative error of at most 0.001.
Values are sent between devices in bfloat16 or wider.
A program may use at most 1 GiB of HBM per device.

```python
import math
import jax
import jax.numpy as jnp
from jax import lax

D = 2048
HEADS = 16
KV_HEADS = 16
HEAD = 128
FF = 1408
EXPERTS = 3
RANK_DIV = 16

MOMENTUM = 0.9
LEARN_RATE = 0.3
FULL_PREC = lax.Precision.HIGHEST


def draw_matrix(rand_key, n_rows, n_cols, n_side):
    sub_keys = jax.random.split(rand_key, 9)
    row_grad = jax.random.uniform(sub_keys[0], (n_rows, 1), jnp.float32, 0.5, 1.5)
    col_grad = jax.random.uniform(sub_keys[1], (1, n_cols), jnp.float32, 0.5, 1.5)
    row_mom = jax.random.uniform(sub_keys[2], (n_rows, 1), jnp.float32, 0.5, 1.5)
    col_mom = jax.random.uniform(sub_keys[3], (1, n_cols), jnp.float32, 0.5, 1.5)
    weight = jax.random.normal(sub_keys[4], (n_rows, n_cols), jnp.float32) * n_rows ** -0.5
    moment = 0.5 * jax.random.normal(sub_keys[5], (n_rows, n_cols), jnp.float32) * row_mom * col_mom
    gradient = (jax.random.normal(sub_keys[6], (n_rows, n_cols), jnp.float32) * row_grad * col_grad).astype(jnp.bfloat16)
    rank_cols = n_side // RANK_DIV
    col_fac = jax.random.uniform(sub_keys[7], (1, rank_cols), jnp.float32, 0.7, 1.3)
    factor = jax.random.normal(sub_keys[8], (n_side, rank_cols), jnp.float32) * col_fac * n_side ** -0.5
    return weight, moment, gradient, factor


def setup_inputs(seed: int = 0, part: int = 0) -> dict:
    part_key = jax.random.fold_in(jax.random.key(seed), part)
    mat_keys = jax.random.split(part_key, 7)
    q_width = HEADS * HEAD
    kv_width = KV_HEADS * HEAD
    drawn = [
        ('wq', draw_matrix(mat_keys[0], D, q_width, q_width)),
        ('wk', draw_matrix(mat_keys[1], D, kv_width, kv_width)),
        ('wv', draw_matrix(mat_keys[2], D, kv_width, kv_width)),
        ('wo', draw_matrix(mat_keys[3], q_width, D, D)),
        ('gate', jax.vmap(lambda sub_key: draw_matrix(sub_key, D, FF, FF))(jax.random.split(mat_keys[4], EXPERTS))),
        ('up', jax.vmap(lambda sub_key: draw_matrix(sub_key, D, FF, FF))(jax.random.split(mat_keys[5], EXPERTS))),
        ('down', jax.vmap(lambda sub_key: draw_matrix(sub_key, FF, D, FF))(jax.random.split(mat_keys[6], EXPERTS))),
    ]
    inputs = {}
    for prefix, arrays in drawn:
        for suffix, drawn_arr in zip(('weight', 'moment', 'grad', 'factor'), arrays):
            inputs[prefix + '_' + suffix] = drawn_arr
    return inputs


def dion_one(weight, moment, gradient, factor):
    mom_grad = moment + gradient.astype(jnp.float32)
    p_tilde = jnp.dot(mom_grad, factor, preferred_element_type=jnp.float32, precision=FULL_PREC)
    gram_mat = jnp.dot(p_tilde.T, p_tilde, preferred_element_type=jnp.float32, precision=FULL_PREC)
    chol_low = jnp.linalg.cholesky(gram_mat)
    p_orth = lax.linalg.triangular_solve(chol_low, p_tilde, left_side=False, lower=True, transpose_a=True)
    r_new = jnp.dot(mom_grad.T, p_orth, preferred_element_type=jnp.float32, precision=FULL_PREC)
    moment_new = mom_grad - (1.0 - MOMENTUM) * jnp.dot(p_orth, r_new.T, preferred_element_type=jnp.float32, precision=FULL_PREC)
    col_norm = jnp.sqrt(jnp.sum(r_new * r_new, axis=0, keepdims=True))
    factor_new = r_new / col_norm
    step_scale = LEARN_RATE * math.sqrt(mom_grad.shape[0] / mom_grad.shape[1])
    weight_new = weight - step_scale * jnp.dot(p_orth, factor_new.T, preferred_element_type=jnp.float32, precision=FULL_PREC)
    return weight_new, moment_new, factor_new


def dion_flip(weight, moment, gradient, factor):
    weight_new, moment_new, factor_new = dion_one(weight.T, moment.T, gradient.T, factor)
    return weight_new.T, moment_new.T, factor_new


def reference(wq_weight, wq_moment, wq_grad, wq_factor, wk_weight, wk_moment, wk_grad, wk_factor, wv_weight, wv_moment, wv_grad, wv_factor, wo_weight, wo_moment, wo_grad, wo_factor, gate_weight, gate_moment, gate_grad, gate_factor, up_weight, up_moment, up_grad, up_factor, down_weight, down_moment, down_grad, down_factor):
    wq_new = dion_one(wq_weight, wq_moment, wq_grad, wq_factor)
    wk_new = dion_one(wk_weight, wk_moment, wk_grad, wk_factor)
    wv_new = dion_one(wv_weight, wv_moment, wv_grad, wv_factor)
    wo_new = dion_one(wo_weight, wo_moment, wo_grad, wo_factor)
    gate_new = lax.map(lambda per_expert: dion_one(per_expert[0], per_expert[1], per_expert[2], per_expert[3]), (gate_weight, gate_moment, gate_grad, gate_factor))
    up_new = lax.map(lambda per_expert: dion_one(per_expert[0], per_expert[1], per_expert[2], per_expert[3]), (up_weight, up_moment, up_grad, up_factor))
    down_new = lax.map(lambda per_expert: dion_flip(per_expert[0], per_expert[1], per_expert[2], per_expert[3]), (down_weight, down_moment, down_grad, down_factor))
    return (wq_new[0], wq_new[1], wq_new[2], wk_new[0], wk_new[1], wk_new[2], wv_new[0], wv_new[1], wv_new[2], wo_new[0], wo_new[1], wo_new[2], gate_new[0], gate_new[1], gate_new[2], up_new[0], up_new[1], up_new[2], down_new[0], down_new[1], down_new[2])
```

```python
import functools
import math
import jax
import jax.numpy as jnp
from jax import lax
from jax.experimental import pallas as pl
from jax.experimental.pallas import tpu as pltpu
from jax.sharding import PartitionSpec as P

MOMENTUM = 0.9
LEARN_RATE = 0.3
F32 = jnp.float32
BF16 = jnp.bfloat16
ND, NG, NE = 4, 6, 3
RD, RE, RX = 128, 96, 88
SQ, SN = 512, 352


def split3(x):
    hi = x.astype(BF16)
    rest = x - hi.astype(F32)
    mid = rest.astype(BF16)
    low = (rest - mid.astype(F32)).astype(BF16)
    return hi, mid, low


def dot(a, b, trans=False):
    dims = (((1,), (1 if trans else 0,)), ((), ()))
    return lax.dot_general(a, b, dims, preferred_element_type=F32)


def mm6(a3, r, b1, b2, b3, trans=False):
    o1 = dot(a3, b1, trans)
    o2 = dot(a3[:2 * r], b2, trans)
    o3 = dot(a3[:r], b3, trans)
    return o1[:r] + ((o1[r:2 * r] + o2[:r]) + ((o1[2 * r:] + o2[r:]) + o3))


def stack3(x):
    return jnp.concatenate(split3(x), axis=0)


def load_sum(m_ref, g_ref, bs_ref, k, rows):
    step = 32

    def body(c, carry):
        sl = pl.ds(pl.multiple_of(c * step, step), step)
        b = m_ref[k, sl, :] + g_ref[k, sl, :].astype(F32)
        b1, b2, b3 = split3(b)
        bs_ref[k, 0, sl, :] = b1
        bs_ref[k, 1, sl, :] = b2
        bs_ref[k, 2, sl, :] = b3
        return carry

    lax.fori_loop(0, rows // step, body, 0)


def sub_bcast(x, t):
    return jnp.broadcast_to(x[t:t + 1, :], (8, 128))


def chol_block(a_ref, li_ref, k, jb, rp):
    lane = lax.broadcasted_iota(jnp.int32, (8, 128), 1)
    sub = lax.broadcasted_iota(jnp.int32, (8, 128), 0)
    base = jb * 8
    row0 = pl.multiple_of(base, 8)
    panel = a_ref[k, pl.ds(row0, 8), :]
    cols = [jnp.take_along_axis(panel, jnp.full((8, 128), 0, jnp.int32) + (base + s), axis=1,
                                mode='promise_in_bounds') for s in range(8)]
    rinv = jnp.zeros((8, 128), F32)
    for t in range(8):
        d = sub_bcast(cols[t], t)
        inv = 1.0 / d
        rinv = jnp.where(sub == t, inv, rinv)
        mult = jnp.where(sub > t, cols[t] * inv, 0.0)
        for s in range(8):
            if s != t:
                cols[s] = cols[s] - mult * sub_bcast(cols[s], t)
        cols[t] = jnp.where(sub == t, 1.0, -mult)
    low = [jnp.where(sub >= s, cols[s], 0.0) for s in range(8)]
    rows = low[0] * sub_bcast(panel, 0)
    for s in range(1, 8):
        rows = rows + low[s] * sub_bcast(panel, s)
    for s in range(8):
        rows = jnp.where(lane == base + s, low[s], rows)
    scale = jnp.sqrt(rinv)
    li_ref[k, pl.ds(row0, 8), :] = jnp.where(lane < base + 8, rows * scale, 0.0)
    f = jnp.where(lane >= base + 8, rows * rinv, 0.0)
    f1, f2, f3 = [v.astype(F32) for v in split3(f)]
    r1, r2, r3 = [v.astype(F32) for v in split3(rows)]
    lhs = jnp.concatenate([f1, f1, f2, f2, f1, f3], axis=0)
    rhs = jnp.concatenate([r1, r2, r1, r2, r3, r1], axis=0)
    upd = lax.dot_general(lhs.T, rhs, (((1,), (0,)), ((), ())), preferred_element_type=F32)
    lane_all = lax.broadcasted_iota(jnp.int32, (rp, 128), 1)
    inside = (lane_all >= base) & (lane_all < base + 8)
    a_ref[k] = jnp.where(inside, 0.0, a_ref[k]) - upd[:rp]


def chol(a_ref, li_ref, ks, nblk, rp):
    def body(jb, carry):
        for k in ks:
            chol_block(a_ref, li_ref, k, jb, rp)
        return carry

    lax.fori_loop(0, nblk, body, 0)


def comm_kernel(*refs):
    names = [
        'md0', 'gd0', 'qd0', 'md1', 'gd1', 'qd1', 'md2', 'gd2', 'qd2', 'md3', 'gd3', 'qd3',
        'mga', 'gga', 'qga', 'mup', 'gup', 'qup', 'mdn', 'gdn', 'qdn',
        'po_d', 'po_g', 'po_n', 'rt_d', 'rt_g', 'rt_n', 'inv_t', 'inv_f',
        'Md', 'Gd', 'Qd', 'Mg', 'Gg', 'Qg', 'Mn', 'Gn', 'Qn', 'Bd', 'Bg', 'Bn',
        'pd', 'pdA', 'pdB', 'pdT', 'pg', 'pgA', 'pgB', 'pgT', 'vn', 'vnA', 'vnB', 'vnT',
        'yd', 'yd1', 'ydh', 'yd2', 'ydT', 'yg', 'yg1', 'ygh', 'yg2', 'ygT', 'yn', 'yn1', 'ynh', 'yn2', 'ynT',
        'Ad', 'Ld', 'Ag', 'Lg', 'An', 'Ln', 'st', 'sr', 'ft', 'fr',
        'lsem', 'zs_d', 'zr_d', 'zs_g', 'zr_g', 'zs_n', 'zr_n', 'ys_d', 'yr_d', 'ys_g', 'yr_g', 'ys_n', 'yr_n',
        'ns', 'nr', 'fs', 'fr2']
    v = dict(zip(names, refs))
    assert len(names) == len(refs)
    z = lax.axis_index('tp')
    f = lax.axis_index('fsdp')
    core = lax.rem(f, 2)
    outer = (z == 0) | (z == 3)
    inner = jnp.logical_not(outer)
    edge = z + 1 - 2 * lax.rem(z, 2)
    mid = 3 - z
    core_p = f + 1 - 2 * core
    y_p = lax.rem(f + 2, 4)

    def lcopy(src, dst, i, j):
        return pltpu.make_async_copy(src, dst, v['lsem'].at[i, j])

    loads = []
    for k in range(ND):
        loads.append([lcopy(v[f'md{k}'], v['Md'].at[k], 0, k), lcopy(v[f'gd{k}'], v['Gd'].at[k], 1, k),
                      lcopy(v[f'qd{k}'], v['Qd'].at[k], 2, k)])
    for e in range(NE):
        loads.append([lcopy(v['mdn'].at[e], v['Mn'].at[e], 0, ND + e), lcopy(v['gdn'].at[e], v['Gn'].at[e], 1, ND + e),
                      lcopy(v['qdn'].at[e], v['Qn'].at[e], 2, ND + e)])
    for k in range(NG):
        m, g, q = ('mga', 'gga', 'qga') if k < 3 else ('mup', 'gup', 'qup')
        loads.append([lcopy(v[m].at[k % 3], v['Mg'].at[k], 0, 7 + k), lcopy(v[g].at[k % 3], v['Gg'].at[k], 1, 7 + k),
                      lcopy(v[q].at[k % 3], v['Qg'].at[k], 2, 7 + k)])
    for group in loads:
        for c in group:
            c.start()

    barrier = pltpu.get_barrier_semaphore()
    for d in range(1, 4):
        pl.semaphore_signal(barrier, inc=1, device_id={'tp': lax.rem(z + d, 4)}, device_id_type=pl.DeviceIdType.MESH)
        pl.semaphore_signal(barrier, inc=1, device_id={'fsdp': lax.rem(f + d, 4)}, device_id_type=pl.DeviceIdType.MESH)
    pl.semaphore_wait(barrier, 6)

    def remote(src, dst, ssem, rsem, dev):
        return pltpu.make_async_remote_copy(src_ref=src, dst_ref=dst, send_sem=ssem, recv_sem=rsem,
                                            device_id=dev, device_id_type=pl.DeviceIdType.MESH)

    def zset(own, a, b, t, ss, rs, rows):
        own, a, b, t, ss, rs = v[own], v[a], v[b], v[t], v[ss], v[rs]

        def cut(ref, k):
            return ref.at[k, pl.ds(0, rows), :]

        def ca(k):
            return remote(cut(own, k), cut(a, k), ss.at[0, k], rs.at[0, k], {'tp': edge})

        def cb(k):
            return remote(cut(own, k), cut(b, k), ss.at[1, k], rs.at[1, k], {'tp': mid})

        def ct(k):
            return remote(cut(t, k), cut(t, k), ss.at[2, k], rs.at[2, k], {'tp': edge})

        def send(k):
            @pl.when(outer)
            def _():
                ca(k).start()

        def s(k):
            @pl.when(inner)
            def _():
                ca(k).wait_recv()
                own[k, :rows] = own[k, :rows] + a[k, :rows]
                cb(k).start()

        def tt(k):
            @pl.when(inner)
            def _():
                cb(k).wait_recv()
                t[k, :rows] = own[k, :rows] + b[k, :rows]
                ct(k).start()

        def w(k):
            @pl.when(outer)
            def _():
                ct(k).wait_recv()

        def fin(k):
            @pl.when(outer)
            def _():
                ca(k).wait_send()

            @pl.when(inner)
            def _():
                cb(k).wait_send()
                ct(k).wait_send()

        return send, s, tt, w, fin

    def yset(own, r1, h, r2, t, ss, rs, half):
        own, r1, h, r2, t, ss, rs = v[own], v[r1], v[h], v[r2], v[t], v[ss], v[rs]
        mine = pl.ds(pl.multiple_of(core * half, 8), half)
        theirs = pl.ds(pl.multiple_of((1 - core) * half, 8), half)

        def c1(k):
            return remote(own.at[k, theirs, :], r1.at[k], ss.at[0, k], rs.at[0, k], {'fsdp': core_p})

        def c2(k):
            return remote(h.at[k], r2.at[k], ss.at[1, k], rs.at[1, k], {'fsdp': y_p})

        def c3(k):
            return remote(t.at[k, mine, :], t.at[k, mine, :], ss.at[2, k], rs.at[2, k], {'fsdp': core_p})

        def y1(k):
            c1(k).start()

        def y2(k):
            c1(k).wait_recv()
            h[k] = own[k, mine, :] + r1[k]
            c2(k).start()

        def y3(k):
            c2(k).wait_recv()
            t[k, mine, :] = h[k] + r2[k]
            c3(k).start()

        def y4(k):
            remote(t.at[k, mine, :], t.at[k, theirs, :], ss.at[2, k], rs.at[2, k], {'fsdp': core_p}).wait_recv()

        def fin(k):
            c1(k).wait_send()
            c2(k).wait_send()
            c3(k).wait_send()

        return y1, y2, y3, y4, fin

    zd = zset('pd', 'pdA', 'pdB', 'pdT', 'zs_d', 'zr_d', RD)
    zg = zset('pg', 'pgA', 'pgB', 'pgT', 'zs_g', 'zr_g', RX)
    zn = zset('vn', 'vnA', 'vnB', 'vnT', 'zs_n', 'zr_n', RX)
    yd = yset('yd', 'yd1', 'ydh', 'yd2', 'ydT', 'ys_d', 'yr_d', RD // 2)
    yg = yset('yg', 'yg1', 'ygh', 'yg2', 'ygT', 'ys_g', 'yr_g', RE // 2)
    yn = yset('yn', 'yn1', 'ynh', 'yn2', 'ynT', 'ys_n', 'yr_n', RE // 2)

    def loop(n, body):
        def go(k, carry):
            body(k)
            return carry
        lax.fori_loop(0, n, go, 0)

    zero_rows = jnp.zeros((RE - RX, SQ), F32)

    def q_stack(q, rp):
        qt = q.T
        if rp != qt.shape[0]:
            qt = jnp.concatenate([qt, jnp.zeros((rp - qt.shape[0], qt.shape[1]), F32)], axis=0)
        return stack3(qt)

    def part_d(k):
        lcopy(v['md0'], v['Md'].at[k], 0, k).wait()
        lcopy(v['gd0'], v['Gd'].at[k], 1, k).wait()
        lcopy(v['qd0'], v['Qd'].at[k], 2, k).wait()
        load_sum(v['Md'], v['Gd'], v['Bd'], k, SQ)
        B = v['Bd']
        v['pd'][k] = mm6(q_stack(v['Qd'][k], RD), RD, B[k, 0], B[k, 1], B[k, 2], True)
        zd[0](k)

    def part_g(k):
        lcopy(v['mga'].at[0], v['Mg'].at[k], 0, 7 + k).wait()
        lcopy(v['gga'].at[0], v['Gg'].at[k], 1, 7 + k).wait()
        lcopy(v['qga'].at[0], v['Qg'].at[k], 2, 7 + k).wait()
        load_sum(v['Mg'], v['Gg'], v['Bg'], k, SQ)
        B = v['Bg']
        v['pg'][k] = mm6(q_stack(v['Qg'][k], RE), RE, B[k, 0], B[k, 1], B[k, 2], True)
        v['pgT'][k, RX:] = zero_rows
        zg[0](k)

    def part_n(k):
        lcopy(v['mdn'].at[0], v['Mn'].at[k], 0, 4 + k).wait()
        lcopy(v['gdn'].at[0], v['Gn'].at[k], 1, 4 + k).wait()
        lcopy(v['qdn'].at[0], v['Qn'].at[k], 2, 4 + k).wait()
        load_sum(v['Mn'], v['Gn'], v['Bn'], k, SN)
        B = v['Bn']
        v['yn'][k] = mm6(q_stack(v['Qn'][k], RE), RE, B[k, 0], B[k, 1], B[k, 2])
        yn[0](k)

    def gram(p3, rp):
        return mm6(p3, rp, p3[:rp], p3[rp:2 * rp], p3[2 * rp:], True)

    def post_d(k):
        zd[3](k)
        p3 = stack3(v['pdT'][k])
        B = v['Bd']
        v['yd'][k, :, :SQ] = mm6(p3, RD, B[k, 0], B[k, 1], B[k, 2])
        v['yd'][k, :, SQ:] = gram(p3, RD)
        yd[0](k)

    def post_g(k):
        zg[3](k)
        p3 = stack3(v['pgT'][k])
        B = v['Bg']
        v['yg'][k, :, :SN] = mm6(p3, RE, B[k, 0], B[k, 1], B[k, 2])
        v['yg'][k, :, SN:384] = jnp.zeros((RE, 384 - SN), F32)
        v['yg'][k, :, 384:384 + RE] = gram(p3, RE)
        v['yg'][k, :, 384 + RE:] = jnp.zeros((RE, 128 - RE), F32)
        yg[0](k)

    def post_n(k):
        yn[3](k)
        p3 = stack3(v['ynT'][k])
        B = v['Bn']
        v['vn'][k, :, :SN] = mm6(p3, RE, B[k, 0], B[k, 1], B[k, 2], True)
        v['vn'][k, :, SN:384] = jnp.zeros((RE, 384 - SN), F32)
        v['vn'][k, :, 384:384 + RE] = gram(p3, RE)
        v['vn'][k, :, 384 + RE:] = jnp.zeros((RE, 128 - RE), F32)
        v['vnT'][k, RX:] = zero_rows
        zn[0](k)

    def orth(l_ref, p_ref, y_ref, po, rt, k, r, rp, width):
        l3 = stack3(l_ref[k, :, :rp])
        q3 = stack3(p_ref[k])
        po[k] = mm6(l3, rp, q3[:rp], q3[rp:2 * rp], q3[2 * rp:])
        y3 = stack3(y_ref[k, :, :width])
        res = mm6(l3, rp, y3[:rp], y3[rp:2 * rp], y3[2 * rp:])
        rt[k] = res
        return jnp.sum(res * res, axis=1, keepdims=True)

    loop(ND, part_d)
    loop(NE, part_n)

    def ph3(k):
        part_g(k)

        @pl.when(k < ND)
        def _():
            zd[1](jnp.minimum(k, ND - 1))

        @pl.when((k >= 1) & (k <= ND))
        def _():
            zd[2](jnp.clip(k - 1, 0, ND - 1))
    loop(NG, ph3)
    loop(NE, yn[1])
    loop(NE, yn[2])
    loop(NE, post_n)

    def ph5(k):
        zg[1](k)

        @pl.when(k >= 1)
        def _():
            zg[2](jnp.maximum(k - 1, 0))

        @pl.when(k < ND)
        def _():
            post_d(jnp.minimum(k, ND - 1))
    loop(NG, ph5)
    zg[2](NG - 1)
    loop(NE, zn[1])
    loop(NE, zn[2])
    loop(ND, yd[1])
    loop(ND, yd[2])
    loop(NG, post_g)

    def take_d(k):
        yd[3](k)
        v['Ad'][k] = v['ydT'][k, :, SQ:]
    loop(ND, take_d)
    chol(v['Ad'], v['Ld'], range(ND), RD // 8, RD)
    loop(NG, yg[1])
    loop(NG, yg[2])

    def take_n(k):
        zn[3](k)
        v['An'][k] = v['vnT'][k, :, 384:]
        v['Ln'][k, RX:] = jnp.zeros((RE - RX, 128), F32)
    loop(NE, take_n)
    chol(v['An'], v['Ln'], range(NE), RX // 8, RE)

    def take_g(k):
        yg[3](k)
        v['Ag'][k] = v['ygT'][k, :, 384:]
        v['Lg'][k, RX:] = jnp.zeros((RE - RX, 128), F32)
    loop(NG, take_g)
    chol(v['Ag'], v['Lg'], range(NG), RX // 8, RE)

    lane_sq = lax.broadcasted_iota(jnp.int32, (128, 128), 1)
    v['st'][...] = jnp.zeros((128, 128), F32)
    v['ft'][...] = jnp.zeros((128, 128), F32)

    def put(ref, col, rp, lane):
        here = lax.broadcasted_iota(jnp.int32, (rp, 128), 1) == lane
        ref[:rp] = jnp.where(here, jnp.broadcast_to(col, (rp, 128)), ref[:rp])

    def orth_d(k):
        put(v['st'], orth(v['Ld'], v['pdT'], v['ydT'], v['po_d'], v['rt_d'], k, RD, RD, SQ), RD, k)
    loop(ND, orth_d)

    def orth_n(k):
        put(v['ft'], orth(v['Ln'], v['ynT'], v['vnT'], v['po_n'], v['rt_n'], k, RX, RE, SN), RE, k)
    loop(NE, orth_n)

    def orth_g(k):
        put(v['st'], orth(v['Lg'], v['pgT'], v['ygT'], v['po_g'], v['rt_g'], k, RX, RE, SN), RE, ND + k)
    loop(NG, orth_g)

    v['sr'][0] = v['st'][...].T[:16]
    v['fr'][0] = v['ft'][...].T[:16]
    copies = []
    for d in range(1, 4):
        copies.append(remote(v['sr'].at[0], v['sr'].at[d], v['ns'].at[d], v['nr'].at[d], {'tp': lax.rem(z + d, 4)}))
        copies.append(remote(v['fr'].at[0], v['fr'].at[d], v['fs'].at[d], v['fr2'].at[d], {'fsdp': lax.rem(f + d, 4)}))
    for c in copies:
        c.start()
    for c in copies:
        c.wait_recv()
    pad = jnp.zeros((112, 128), F32)
    tot_t = (v['sr'][0] + v['sr'][2]) + (v['sr'][1] + v['sr'][3])
    tot_f = (v['fr'][0] + v['fr'][2]) + (v['fr'][1] + v['fr'][3])
    inv_t = jnp.where(tot_t > 0.0, 1.0 / jnp.sqrt(tot_t), 0.0)
    inv_f = jnp.where(tot_f > 0.0, 1.0 / jnp.sqrt(tot_f), 0.0)
    v['inv_t'][...] = jnp.concatenate([inv_t, pad], axis=0).T
    v['inv_f'][...] = jnp.concatenate([inv_f, pad], axis=0).T

    for c in copies:
        c.wait_send()
    loop(ND, zd[4])
    loop(NG, zg[4])
    loop(NE, zn[4])
    loop(ND, yd[4])
    loop(NG, yg[4])
    loop(NE, yn[4])


def update_kernel(*refs):
    names = ['po_d', 'po_g', 'po_n', 'rt_d', 'rt_g', 'rt_n', 'inv_t', 'inv_f']
    ins = []
    for g in ('d0', 'd1', 'd2', 'd3', 'ga', 'up', 'dn'):
        ins += [f'x{g}', f'm{g}', f'g{g}']
    outs = []
    for g in ('d0', 'd1', 'd2', 'd3', 'ga', 'up', 'dn'):
        outs += [f'X{g}', f'M{g}', f'Q{g}']
    scr = ['xd', 'md', 'gd', 'xg', 'mg', 'gg', 'xn', 'mn', 'gn', 'lsem', 'osem']
    v = dict(zip(names + ins + outs + scr, refs))
    assert len(names + ins + outs + scr) == len(refs)
    tags = [('d0', None), ('d1', None), ('d2', None), ('d3', None)] + [('ga', e) for e in range(3)] + \
        [('up', e) for e in range(3)] + [('dn', e) for e in range(3)]

    def at(name, e):
        return v[name] if e is None else v[name].at[e]

    def slot(i):
        if i < 4:
            return 'd', i
        if i < 10:
            return 'g', i - 4
        return 'n', i - 10

    loads, stores = [], []
    for i, (tag, e) in enumerate(tags):
        g, k = slot(i)
        loads.append([pltpu.make_async_copy(at(c + tag, e), v[c + g].at[k], v['lsem'].at[j, i])
                      for j, c in enumerate(('m', 'g', 'x'))])
        stores.append([pltpu.make_async_copy(v[c.lower() + g].at[k], at(c + tag, e), v['osem'].at[j, i])
                       for j, c in enumerate(('M', 'X'))])
    for group in loads:
        for c in group:
            c.start()

    def pack(x):
        a, b, c = split3(x)
        return jnp.concatenate([a, b], axis=1), jnp.concatenate([a, c], axis=1)

    def packs(y):
        a, b, c = split3(y)
        return (jnp.concatenate([a, b], axis=0), jnp.concatenate([b, a], axis=0), jnp.concatenate([c, a], axis=0))

    def pad(x):
        if x.shape[0] == 128:
            return x
        return jnp.concatenate([x, jnp.zeros((128 - x.shape[0], x.shape[1]), F32)], axis=0)

    def prod(lhs, rhs):
        return dot(lhs[0], rhs[0]) + (dot(lhs[0], rhs[1]) + dot(lhs[1], rhs[2]))

    for i, (tag, e) in enumerate(tags):
        g, k = slot(i)
        pt = pad(v['po_' + g][k])
        rt = pad(v['rt_' + g][k])
        inv = v['inv_f'][:, k:k + 1] if g == 'n' else v['inv_t'][:, i:i + 1]
        qt = rt * jnp.broadcast_to(inv, rt.shape)
        flip = g == 'n'
        for c in loads[i]:
            c.wait()
        m, gr, x = v['m' + g], v['g' + g], v['x' + g]
        eta = LEARN_RATE * (math.sqrt(2048 / 1408) if i >= 4 else 1.0)
        if flip:
            q = qt.T
            rhs = packs(pt)
            m[k] = m[k] + gr[k].astype(F32) - (1.0 - MOMENTUM) * prod(pack(rt.T), rhs)
            stores[i][0].start()
            x[k] = x[k] - eta * prod(pack(q), rhs)
            stores[i][1].start()
        else:
            lhs = pack(pt.T)
            m[k] = m[k] + gr[k].astype(F32) - (1.0 - MOMENTUM) * prod(lhs, packs(rt))
            stores[i][0].start()
            x[k] = x[k] - eta * prod(lhs, packs(qt))
            stores[i][1].start()
            q = qt.T
        if e is None:
            v['Q' + tag][...] = q
        else:
            v['Q' + tag][e] = q[:, :RX]
    for group in stores:
        for c in group:
            c.wait()


def vm(*shape, dtype=F32):
    return pltpu.VMEM(shape, dtype)


def solution(mesh):
    dense_w = P(('layer', 'fsdp'), 'tp')
    dense_f = P(('layer', 'tp'), None)
    stack_w = P('layer', 'fsdp', 'tp')
    stack_f = P('layer', 'tp', None)
    down_f = P('layer', 'fsdp', None)
    in_specs = (dense_w, dense_w, dense_w, dense_f) * 4 + (stack_w, stack_w, stack_w, stack_f) * 2 + (stack_w, stack_w, stack_w, down_f)
    out_specs = (dense_w, dense_w, dense_f) * 4 + (stack_w, stack_w, stack_f) * 2 + (stack_w, stack_w, down_f)
    dma = pltpu.SemaphoreType.DMA
    anyspec = pl.BlockSpec(memory_space=pl.ANY)
    vspec = pl.BlockSpec(memory_space=pltpu.VMEM)

    def local_step(*blocks):
        mats = [blocks[4 * i:4 * i + 4] for i in range(7)]
        first = []
        for x, m, g, q in mats:
            first += [m, g, q]
        scratch = [
            vm(ND, SQ, SQ), vm(ND, SQ, SQ, dtype=BF16), vm(ND, SQ, RD),
            vm(NG, SQ, SN), vm(NG, SQ, SN, dtype=BF16), vm(NG, SN, RX),
            vm(NE, SN, SQ), vm(NE, SN, SQ, dtype=BF16), vm(NE, SN, RX),
            vm(ND, 3, SQ, SQ, dtype=BF16), vm(NG, 3, SQ, SN, dtype=BF16), vm(NE, 3, SN, SQ, dtype=BF16)]
        scratch += [vm(ND, RD, SQ)] * 4 + [vm(NG, RE, SQ)] * 4 + [vm(NE, RE, SQ)] * 4
        for n, rp, w in ((ND, RD, SQ + 128), (NG, RE, 512), (NE, RE, 512)):
            scratch += [vm(n, rp, w), vm(n, rp // 2, w), vm(n, rp // 2, w), vm(n, rp // 2, w), vm(n, rp, w)]
        for n, rp in ((ND, RD), (NG, RE), (NE, RE)):
            scratch += [vm(n, rp, 128), vm(n, rp, 128)]
        scratch += [vm(128, 128), vm(4, 16, 128), vm(128, 128), vm(4, 16, 128)]
        scratch += [dma((3, 13))]
        scratch += [dma((3, n)) for n in (ND, ND, NG, NG, NE, NE)] * 2
        scratch += [dma((4,))] * 4
        shapes = [(ND, RD, SQ), (NG, RE, SQ), (NE, RE, SQ), (ND, RD, SQ), (NG, RE, SN), (NE, RE, SN), (128, 128), (128, 128)]
        mids = pl.pallas_call(
            comm_kernel,
            out_shape=[jax.ShapeDtypeStruct(s, F32) for s in shapes],
            in_specs=[anyspec] * 21,
            out_specs=[vspec] * 8,
            scratch_shapes=scratch,
            name='comm',
            compiler_params=pltpu.CompilerParams(collective_id=0, has_side_effects=True, vmem_limit_bytes=64 * 1024 * 1024 - 65536),
        )(*first)
        second, shapes2, ospecs = [], [], []
        for x, m, g, q in mats:
            second += [x, m, g]
            shapes2 += [x, m, q]
            ospecs += [anyspec, anyspec, vspec]
        res = pl.pallas_call(
            update_kernel,
            out_shape=[jax.ShapeDtypeStruct(a.shape, F32) for a in shapes2],
            in_specs=[vspec] * 8 + [anyspec] * 21,
            out_specs=ospecs,
            scratch_shapes=[vm(ND, SQ, SQ), vm(ND, SQ, SQ), vm(ND, SQ, SQ, dtype=BF16),
                            vm(NG, SQ, SN), vm(NG, SQ, SN), vm(NG, SQ, SN, dtype=BF16),
                            vm(NE, SN, SQ), vm(NE, SN, SQ), vm(NE, SN, SQ, dtype=BF16), dma((3, 13)), dma((2, 13))],
            name='update',
            compiler_params=pltpu.CompilerParams(vmem_limit_bytes=64 * 1024 * 1024 - 65536),
        )(*mids, *second)
        return tuple(res)

    return jax.shard_map(local_step, mesh=mesh, in_specs=in_specs, out_specs=out_specs, check_vma=False)
```

```python
import functools
import math
import jax
import jax.numpy as jnp
from jax import lax
from jax.experimental import pallas as pl
from jax.experimental.pallas import tpu as pltpu
from jax.sharding import PartitionSpec as P

MOMENTUM = 0.9
LEARN_RATE = 0.3
VMEM_MAX = 58 * 1024 * 1024
F32 = jnp.float32
BF16 = jnp.bfloat16
ND, NG, NE = 4, 6, 3
RD, RE, RX = 128, 96, 88
SQ, SN = 512, 352


def split3(x):
    hi = x.astype(BF16)
    rest = x - hi.astype(F32)
    mid = rest.astype(BF16)
    low = (rest - mid.astype(F32)).astype(BF16)
    return hi, mid, low


def dot(a, b, trans=False):
    dims = (((1,), (1 if trans else 0,)), ((), ()))
    return lax.dot_general(a, b, dims, preferred_element_type=F32)


def mm6(a3, r, b1, b2, b3, trans=False):
    o1 = dot(a3, b1, trans)
    o2 = dot(a3[:2 * r], b2, trans)
    o3 = dot(a3[:r], b3, trans)
    return o1[:r] + ((o1[r:2 * r] + o2[:r]) + ((o1[2 * r:] + o2[r:]) + o3))


def stack3(x):
    return jnp.concatenate(split3(x), axis=0)


def load_sum(m_ref, g_ref, bs_ref, k, rows):
    step = 32

    def body(c, carry):
        sl = pl.ds(pl.multiple_of(c * step, step), step)
        b = m_ref[k, sl, :] + g_ref[k, sl, :].astype(F32)
        b1, b2, b3 = split3(b)
        bs_ref[k, 0, sl, :] = b1
        bs_ref[k, 1, sl, :] = b2
        bs_ref[k, 2, sl, :] = b3
        return carry

    lax.fori_loop(0, rows // step, body, 0)


def sub_bcast(x, t):
    return jnp.broadcast_to(x[t:t + 1, :], (8, 128))


def chol_step(a_ref, li_ref, ks, jb, rp):
    lane = lax.broadcasted_iota(jnp.int32, (8, 128), 1)
    sub = lax.broadcasted_iota(jnp.int32, (8, 128), 0)
    base = jb * 8
    row0 = pl.multiple_of(base, 8)
    n = range(len(ks))
    panel = [a_ref[k, pl.ds(row0, 8), :] for k in ks]
    idx = [jnp.full((8, 128), 0, jnp.int32) + (base + s) for s in range(8)]
    cols = [[jnp.take_along_axis(panel[i], idx[s], axis=1, mode='promise_in_bounds') for s in range(8)] for i in n]
    rinv = [jnp.zeros((8, 128), F32) for i in n]
    for t in range(8):
        inv = [1.0 / sub_bcast(cols[i][t], t) for i in n]
        for i in n:
            rinv[i] = jnp.where(sub == t, inv[i], rinv[i])
        mult = [jnp.where(sub > t, cols[i][t] * inv[i], 0.0) for i in n]
        for i in n:
            for s in range(8):
                if s != t:
                    cols[i][s] = cols[i][s] - mult[i] * sub_bcast(cols[i][s], t)
            cols[i][t] = jnp.where(sub == t, 1.0, -mult[i])
    low = [[jnp.where(sub >= s, cols[i][s], 0.0) for s in range(8)] for i in n]
    rows = []
    for i in n:
        r = low[i][0] * sub_bcast(panel[i], 0)
        for s in range(1, 8):
            r = r + low[i][s] * sub_bcast(panel[i], s)
        for s in range(8):
            r = jnp.where(lane == base + s, low[i][s], r)
        rows.append(r)
    upd = []
    for i in n:
        f = jnp.where(lane >= base + 8, rows[i] * rinv[i], 0.0)
        f1, f2, f3 = [x.astype(F32) for x in split3(f)]
        r1, r2, r3 = [x.astype(F32) for x in split3(rows[i])]
        lhs = jnp.concatenate([f1, f1, f2, f2, f1, f3], axis=0)
        rhs = jnp.concatenate([r1, r2, r1, r2, r3, r1], axis=0)
        upd.append(lax.dot_general(lhs.T, rhs, (((1,), (0,)), ((), ())), preferred_element_type=F32))
    lane_all = lax.broadcasted_iota(jnp.int32, (rp, 128), 1)
    inside = (lane_all >= base) & (lane_all < base + 8)
    for i in n:
        a_ref[ks[i]] = jnp.where(inside, 0.0, a_ref[ks[i]]) - upd[i][:rp]
    for i in n:
        li_ref[ks[i], pl.ds(row0, 8), :] = jnp.where(lane < base + 8, rows[i] * jnp.sqrt(rinv[i]), 0.0)


def chol(a_ref, li_ref, ks, nblk, rp, duties=()):
    def body(jb, carry):
        chol_step(a_ref, li_ref, ks, jb, rp)
        for at, duty in duties:
            pl.when(jb == at)(duty)
        return carry

    lax.fori_loop(0, nblk, body, 0)


def comm_kernel(*refs):
    names = [
        'md0', 'gd0', 'qd0', 'md1', 'gd1', 'qd1', 'md2', 'gd2', 'qd2', 'md3', 'gd3', 'qd3',
        'mga', 'gga', 'qga', 'mup', 'gup', 'qup', 'mdn', 'gdn', 'qdn',
        'po_d', 'po_g', 'po_n', 'rt_d', 'rt_g', 'rt_n', 'inv_t', 'inv_f',
        'Md', 'Gd', 'Qd', 'Mg', 'Gg', 'Qg', 'Mn', 'Gn', 'Qn', 'Bd', 'Bg', 'Bn',
        'pd', 'pdT', 'pdB', 'pg', 'pgT', 'pgB', 'vn', 'vnT', 'vnB',
        'yd', 'yd1', 'yd2', 'ydT', 'yg', 'yg1', 'yg2', 'ygT', 'yn', 'yn1', 'yn2', 'ynT',
        'Ad', 'Ld', 'Ag', 'Lg', 'An', 'Ln', 'st', 'sr', 'ft', 'fr',
        'lsem', 'zs_d', 'zr_d', 'zs_g', 'zr_g', 'zs_n', 'zr_n', 'ys_d', 'yr_d', 'ys_g', 'yr_g', 'ys_n', 'yr_n',
        'ns', 'nr', 'fs', 'fr2']
    v = dict(zip(names, refs))
    assert len(names) == len(refs)
    z = lax.axis_index('tp')
    f = lax.axis_index('fsdp')
    core = lax.rem(f, 2)
    outer = (z == 0) | (z == 3)
    inner = jnp.logical_not(outer)
    edge = z + 1 - 2 * lax.rem(z, 2)
    mid = 3 - z
    core_p = f + 1 - 2 * core
    y_p = lax.rem(f + 2, 4)

    def lcopy(src, dst, i, j):
        return pltpu.make_async_copy(src, dst, v['lsem'].at[i, j])

    loads = []
    for k in range(ND):
        loads.append([lcopy(v[f'md{k}'], v['Md'].at[k], 0, k), lcopy(v[f'gd{k}'], v['Gd'].at[k], 1, k),
                      lcopy(v[f'qd{k}'], v['Qd'].at[k], 2, k)])
    for e in range(NE):
        loads.append([lcopy(v['mdn'].at[e], v['Mn'].at[e], 0, ND + e), lcopy(v['gdn'].at[e], v['Gn'].at[e], 1, ND + e),
                      lcopy(v['qdn'].at[e], v['Qn'].at[e], 2, ND + e)])
    for k in range(NG):
        m, g, q = ('mga', 'gga', 'qga') if k < 3 else ('mup', 'gup', 'qup')
        loads.append([lcopy(v[m].at[k % 3], v['Mg'].at[k], 0, 7 + k), lcopy(v[g].at[k % 3], v['Gg'].at[k], 1, 7 + k),
                      lcopy(v[q].at[k % 3], v['Qg'].at[k], 2, 7 + k)])
    for group in loads:
        for c in group:
            c.start()

    barrier = pltpu.get_barrier_semaphore()
    for d in range(1, 4):
        pl.semaphore_signal(barrier, inc=1, device_id={'tp': lax.rem(z + d, 4)}, device_id_type=pl.DeviceIdType.MESH)
        pl.semaphore_signal(barrier, inc=1, device_id={'fsdp': lax.rem(f + d, 4)}, device_id_type=pl.DeviceIdType.MESH)
    pl.semaphore_wait(barrier, 6)

    def remote(src, dst, ssem, rsem, dev):
        return pltpu.make_async_remote_copy(src_ref=src, dst_ref=dst, send_sem=ssem, recv_sem=rsem,
                                            device_id=dev, device_id_type=pl.DeviceIdType.MESH)

    def zpiece(own, t, b, ss, rs, i, k, row0, rows, col0, cols):
        own, t, b = [v[x].at[k, pl.ds(row0, rows), pl.ds(col0, cols)] for x in (own, t, b)]
        ss, rs = v[ss], v[rs]
        def ca():
            return remote(own, t, ss.at[0, i], rs.at[0, i], {'tp': edge})
        def cb():
            return remote(own, b, ss.at[1, i], rs.at[1, i], {'tp': mid})
        def ct():
            return remote(t, t, ss.at[2, i], rs.at[2, i], {'tp': edge})

        def send():
            @pl.when(outer)
            def _():
                ca().start()

        def half():
            @pl.when(inner)
            def _():
                ca().wait_recv()
                own[...] = own[...] + t[...]
                cb().start()

        def total():
            @pl.when(inner)
            def _():
                cb().wait_recv()
                t[...] = own[...] + b[...]
                ct().start()

        def take():
            @pl.when(outer)
            def _():
                ct().wait_recv()

        def done():
            @pl.when(outer)
            def _():
                ca().wait_send()

            @pl.when(inner)
            def _():
                cb().wait_send()
                ct().wait_send()

        return send, half, total, take, done

    def yset(own, r1, r2, t, ss, rs, half):
        own, r1, r2, t, ss, rs = v[own], v[r1], v[r2], v[t], v[ss], v[rs]
        h = r1
        mine = pl.ds(pl.multiple_of(core * half, 8), half)
        theirs = pl.ds(pl.multiple_of((1 - core) * half, 8), half)

        def c1(k):
            return remote(own.at[k, theirs, :], r1.at[k], ss.at[0, k], rs.at[0, k], {'fsdp': core_p})

        def c2(k):
            return remote(h.at[k], r2.at[k], ss.at[1, k], rs.at[1, k], {'fsdp': y_p})

        def c3(k):
            return remote(t.at[k, mine, :], t.at[k, mine, :], ss.at[2, k], rs.at[2, k], {'fsdp': core_p})

        def y1(k):
            c1(k).start()

        def y2(k):
            c1(k).wait_recv()
            h[k] = own[k, mine, :] + r1[k]
            c2(k).start()

        def y3(k):
            c2(k).wait_recv()
            t[k, mine, :] = h[k] + r2[k]
            c3(k).start()

        def y4(k):
            remote(t.at[k, mine, :], t.at[k, theirs, :], ss.at[2, k], rs.at[2, k], {'fsdp': core_p}).wait_recv()

        def fin(k):
            c1(k).wait_send()
            c2(k).wait_send()
            c3(k).wait_send()

        return y1, y2, y3, y4, fin

    Z = []
    where = {}
    for k in range(ND):
        for h in range(2):
            where['d', k, h] = len(Z)
            Z.append(zpiece('pd', 'pdT', 'pdB', 'zs_d', 'zr_d', 2 * k + h, k, h * 64, 64, 0, SQ))
    for k in range(NE):
        where['G', k] = len(Z)
        Z.append(zpiece('vn', 'vnT', 'vnB', 'zs_n', 'zr_n', k, k, 0, RX, 384, 128))
    for k in range(NG):
        where['g', k] = len(Z)
        Z.append(zpiece('pg', 'pgT', 'pgB', 'zs_g', 'zr_g', k, k, 0, RX, 0, SQ))
    for k in range(NE):
        where['Y', k] = len(Z)
        Z.append(zpiece('vn', 'vnT', 'vnB', 'zs_n', 'zr_n', NE + k, k, 0, RX, 0, 384))


    def A(*key):
        Z[where[key]][0]()

    def S(n):
        Z[n][1]()

    def T(n):
        Z[n][2]()

    def W(*key):
        Z[where[key]][3]()

    yd = yset('yd', 'yd1', 'yd2', 'ydT', 'ys_d', 'yr_d', RD // 2)
    yg = yset('yg', 'yg1', 'yg2', 'ygT', 'ys_g', 'yr_g', RE // 2)
    yn = yset('yn', 'yn1', 'yn2', 'ynT', 'ys_n', 'yr_n', RE // 2)

    def loop(n, body):
        def go(k, carry):
            body(k)
            return carry
        lax.fori_loop(0, n, go, 0)

    zero_rows = jnp.zeros((RE - RX, SQ), F32)

    def q_stack(qt, rp):
        if rp != qt.shape[0]:
            qt = jnp.concatenate([qt, jnp.zeros((rp - qt.shape[0], qt.shape[1]), F32)], axis=0)
        return stack3(qt)

    def part_d(k):
        lcopy(v['md0'], v['Md'].at[k], 0, k).wait()
        lcopy(v['gd0'], v['Gd'].at[k], 1, k).wait()
        lcopy(v['qd0'], v['Qd'].at[k], 2, k).wait()
        load_sum(v['Md'], v['Gd'], v['Bd'], k, SQ)
        B = v['Bd']
        v['pd'][k] = mm6(q_stack(v['Qd'][k].T, RD), RD, B[k, 0], B[k, 1], B[k, 2], True)
        A('d', k, 0)
        A('d', k, 1)

    def part_g(k):
        lcopy(v['mga'].at[0], v['Mg'].at[k], 0, 7 + k).wait()
        lcopy(v['gga'].at[0], v['Gg'].at[k], 1, 7 + k).wait()
        lcopy(v['qga'].at[0], v['Qg'].at[k], 2, 7 + k).wait()
        load_sum(v['Mg'], v['Gg'], v['Bg'], k, SN)
        B = v['Bg']
        v['pg'][k] = mm6(q_stack(v['Qg'][k], RE), RE, B[k, 0], B[k, 1], B[k, 2])
        v['pgT'][k, RX:] = zero_rows

    def part_n(k):
        lcopy(v['mdn'].at[0], v['Mn'].at[k], 0, 4 + k).wait()
        lcopy(v['gdn'].at[0], v['Gn'].at[k], 1, 4 + k).wait()
        lcopy(v['qdn'].at[0], v['Qn'].at[k], 2, 4 + k).wait()
        load_sum(v['Mn'], v['Gn'], v['Bn'], k, SN)
        B = v['Bn']
        v['yn'][k] = mm6(q_stack(v['Qn'][k], RE), RE, B[k, 0], B[k, 1], B[k, 2])
        yn[0](k)

    def gram(p3, rp):
        return mm6(p3, rp, p3[:rp], p3[rp:2 * rp], p3[2 * rp:], True)

    def post_d(k):
        W('d', k, 0)
        W('d', k, 1)
        p3 = stack3(v['pdT'][k])
        B = v['Bd']
        v['yd'][k, :, :SQ] = mm6(p3, RD, B[k, 0], B[k, 1], B[k, 2])
        v['yd'][k, :, SQ:] = gram(p3, RD)
        yd[0](k)

    def post_g(k):
        W('g', k)
        p3 = stack3(v['pgT'][k])
        B = v['Bg']
        v['yg'][k, :, :SN] = mm6(p3, RE, B[k, 0], B[k, 1], B[k, 2], True)
        v['yg'][k, :, SN:384] = jnp.zeros((RE, 384 - SN), F32)
        v['yg'][k, :, 384:384 + RE] = gram(p3, RE)
        v['yg'][k, :, 384 + RE:] = jnp.zeros((RE, 128 - RE), F32)
        yg[0](k)

    def post_n(k):
        yn[3](k)
        p3 = stack3(v['ynT'][k])
        B = v['Bn']
        v['vn'][k, :, :SN] = mm6(p3, RE, B[k, 0], B[k, 1], B[k, 2], True)
        v['vn'][k, :, SN:384] = jnp.zeros((RE, 384 - SN), F32)
        v['vn'][k, :, 384:384 + RE] = gram(p3, RE)
        v['vn'][k, :, 384 + RE:] = jnp.zeros((RE, 128 - RE), F32)
        v['vnT'][k, RX:] = zero_rows
        A('G', k)

    def orth_p(l_ref, p_ref, po, k, rp):
        l3 = stack3(l_ref[k, :, :rp])
        q3 = stack3(p_ref[k])
        po[k] = mm6(l3, rp, q3[:rp], q3[rp:2 * rp], q3[2 * rp:])

    def orth_r(l_ref, y_ref, rt, k, rp, width, norm, lane):
        l3 = stack3(l_ref[k, :, :rp])
        y3 = stack3(y_ref[k, :, :width])
        res = mm6(l3, rp, y3[:rp], y3[rp:2 * rp], y3[2 * rp:])
        rt[k] = res
        col = jnp.sum(res * res, axis=1, keepdims=True)
        here = lax.broadcasted_iota(jnp.int32, (rp, 128), 1) == lane
        norm[:rp] = jnp.where(here, jnp.broadcast_to(col, (rp, 128)), norm[:rp])

    def orth_d(k):
        orth_p(v['Ld'], v['pdT'], v['po_d'], k, RD)
        orth_r(v['Ld'], v['ydT'], v['rt_d'], k, RD, SQ, v['st'], k)

    def orth_g(k):
        orth_p(v['Lg'], v['pgT'], v['po_g'], k, RE)
        orth_r(v['Lg'], v['ygT'], v['rt_g'], k, RE, SN, v['st'], ND + k)

    def take_d(k):
        yd[3](k)
        v['Ad'][k] = v['ydT'][k, :, SQ:]

    def take_g(k):
        yg[3](k)
        v['Ag'][k] = v['ygT'][k, :, 384:]
        v['Lg'][k, RX:] = jnp.zeros((RE - RX, 128), F32)

    def take_n(k):
        W('G', k)
        v['An'][k] = v['vnT'][k, :, 384:]
        v['Ln'][k, RX:] = jnp.zeros((RE - RX, 128), F32)

    def ST(n):
        def go():
            S(n)
            T(n - 1)
        return go

    v['st'][...] = jnp.zeros((128, 128), F32)
    v['ft'][...] = jnp.zeros((128, 128), F32)


    for k in range(ND):
        part_d(k)
    part_n(0)
    part_n(1)
    S(0)
    part_n(2)
    part_g(0)
    part_g(1)
    ST(1)()
    for k in range(NE):
        yn[1](k)
    part_g(2)
    part_g(3)
    ST(2)()
    for k in range(NE):
        yn[2](k)
    ST(3)()
    for k in range(NE):
        post_n(k)
    for k in range(4):
        A('g', k)
    ST(4)()
    part_g(4)
    part_g(5)
    for k in range(4, NG):
        A('g', k)
    for k in range(NE):
        A('Y', k)
    ST(5)()
    post_d(0)
    ST(6)()
    post_d(1)
    yd[1](0)
    ST(7)()
    post_d(2)
    yd[1](1)
    yd[2](0)
    for n in (8, 9, 10):
        ST(n)()
    T(10)
    for k in range(NE):
        take_n(k)
    chol(v['An'], v['Ln'], [0, 1, 2], RX // 8, RE, [(2, lambda: S(11)), (9, ST(12))])
    post_d(3)
    yd[1](2)
    yd[2](1)
    for k in range(NE):
        orth_p(v['Ln'], v['ynT'], v['po_n'], k, RE)
    yd[1](3)
    yd[2](2)
    ST(13)()
    post_g(0)
    yd[2](3)
    for k in range(ND):
        take_d(k)
    chol(v['Ad'], v['Ld'], [0, 1, 2, 3], RD // 8, RD, [(4, ST(14)), (11, ST(15))])
    post_g(1)
    yg[1](0)
    ST(16)()
    post_g(2)
    yg[1](1)
    yg[2](0)
    orth_d(0)
    yg[1](2)
    yg[2](1)
    ST(17)()
    post_g(3)
    yg[2](2)
    for k in range(3):
        take_g(k)
    chol(v['Ag'], v['Lg'], [0, 1, 2], RX // 8, RE, [(3, ST(18)), (8, ST(19))])
    post_g(4)
    T(19)
    yg[1](3)
    post_g(5)
    orth_d(1)
    yg[1](4)
    yg[2](3)
    orth_d(2)
    yg[1](5)
    yg[2](4)
    orth_d(3)
    orth_g(0)
    yg[2](5)
    orth_g(1)
    orth_g(2)
    for k in range(3, NG):
        take_g(k)
    chol(v['Ag'], v['Lg'], [3, 4, 5], RX // 8, RE)
    for k in range(NE):
        W('Y', k)
        orth_r(v['Ln'], v['vnT'], v['rt_n'], k, RE, SN, v['ft'], k)
    for k in range(3, NG):
        orth_g(k)

    v['sr'][0] = v['st'][...].T[:16]
    v['fr'][0] = v['ft'][...].T[:16]
    copies = []
    for d in range(1, 4):
        copies.append(remote(v['sr'].at[0], v['sr'].at[d], v['ns'].at[d], v['nr'].at[d], {'tp': lax.rem(z + d, 4)}))
        copies.append(remote(v['fr'].at[0], v['fr'].at[d], v['fs'].at[d], v['fr2'].at[d], {'fsdp': lax.rem(f + d, 4)}))
    for c in copies:
        c.start()
    for c in copies:
        c.wait_recv()
    pad = jnp.zeros((112, 128), F32)
    tot_t = (v['sr'][0] + v['sr'][2]) + (v['sr'][1] + v['sr'][3])
    tot_f = (v['fr'][0] + v['fr'][2]) + (v['fr'][1] + v['fr'][3])
    inv_t = jnp.where(tot_t > 0.0, 1.0 / jnp.sqrt(tot_t), 0.0)
    inv_f = jnp.where(tot_f > 0.0, 1.0 / jnp.sqrt(tot_f), 0.0)
    v['inv_t'][...] = jnp.concatenate([inv_t, pad], axis=0).T
    v['inv_f'][...] = jnp.concatenate([inv_f, pad], axis=0).T

    for c in copies:
        c.wait_send()
    for piece in Z:
        piece[4]()
    loop(ND, yd[4])
    loop(NG, yg[4])
    loop(NE, yn[4])


def update_kernel(*refs):
    names = ['po_d', 'po_g', 'po_n', 'rt_d', 'rt_g', 'rt_n', 'inv_t', 'inv_f']
    ins = []
    for g in ('d0', 'd1', 'd2', 'd3', 'ga', 'up', 'dn'):
        ins += [f'x{g}', f'm{g}', f'g{g}']
    outs = []
    for g in ('d0', 'd1', 'd2', 'd3', 'ga', 'up', 'dn'):
        outs += [f'X{g}', f'M{g}', f'Q{g}']
    scr = ['xd', 'md', 'gd', 'xg', 'mg', 'gg', 'xn', 'mn', 'gn', 'lsem', 'osem']
    v = dict(zip(names + ins + outs + scr, refs))
    assert len(names + ins + outs + scr) == len(refs)
    tags = [('d0', None), ('d1', None), ('d2', None), ('d3', None)] + [('ga', e) for e in range(3)] + \
        [('up', e) for e in range(3)] + [('dn', e) for e in range(3)]

    def at(name, e):
        return v[name] if e is None else v[name].at[e]

    def slot(i):
        if i < 4:
            return 'd', i
        if i < 10:
            return 'g', i - 4
        return 'n', i - 10

    loads, stores = [], []
    for i, (tag, e) in enumerate(tags):
        g, k = slot(i)
        loads.append([pltpu.make_async_copy(at(c + tag, e), v[c + g].at[k], v['lsem'].at[j, i])
                      for j, c in enumerate(('m', 'g', 'x'))])
        stores.append([pltpu.make_async_copy(v[c.lower() + g].at[k], at(c + tag, e), v['osem'].at[j, i])
                       for j, c in enumerate(('M', 'X'))])
    for group in loads:
        for c in group:
            c.start()

    def pack(x):
        a, b, c = split3(x)
        return jnp.concatenate([a, b], axis=1), jnp.concatenate([a, c], axis=1)

    def packs(y):
        a, b, c = split3(y)
        return (jnp.concatenate([a, b], axis=0), jnp.concatenate([b, a], axis=0), jnp.concatenate([c, a], axis=0))

    def pad(x):
        if x.shape[0] == 128:
            return x
        return jnp.concatenate([x, jnp.zeros((128 - x.shape[0], x.shape[1]), F32)], axis=0)

    def prod(lhs, rhs):
        return dot(lhs[0], rhs[0]) + (dot(lhs[0], rhs[1]) + dot(lhs[1], rhs[2]))

    for i, (tag, e) in enumerate(tags):
        g, k = slot(i)
        pt = pad(v['po_' + g][k])
        rt = pad(v['rt_' + g][k])
        inv = v['inv_f'][:, k:k + 1] if g == 'n' else v['inv_t'][:, i:i + 1]
        qt = rt * jnp.broadcast_to(inv, rt.shape)
        flip = g != 'd'
        for c in loads[i]:
            c.wait()
        m, gr, x = v['m' + g], v['g' + g], v['x' + g]
        eta = LEARN_RATE * (math.sqrt(2048 / 1408) if i >= 4 else 1.0)
        if flip:
            q = qt
            rhs = packs(pt)
            m[k] = m[k] + gr[k].astype(F32) - (1.0 - MOMENTUM) * prod(pack(rt.T), rhs)
            stores[i][0].start()
            x[k] = x[k] - eta * prod(pack(qt.T), rhs)
            stores[i][1].start()
        else:
            lhs = pack(pt.T)
            m[k] = m[k] + gr[k].astype(F32) - (1.0 - MOMENTUM) * prod(lhs, packs(rt))
            stores[i][0].start()
            x[k] = x[k] - eta * prod(lhs, packs(qt))
            stores[i][1].start()
            q = qt.T
        if e is None:
            v['Q' + tag][...] = q
        else:
            v['Q' + tag][e] = q[:RX]
    for group in stores:
        for c in group:
            c.wait()


def vm(*shape, dtype=F32):
    return pltpu.VMEM(shape, dtype)


def solution(mesh):
    dense_w = P(('layer', 'fsdp'), 'tp')
    dense_f = P(('layer', 'tp'), None)
    stack_w = P('layer', 'fsdp', 'tp')
    stack_f = P('layer', 'tp', None)
    down_f = P('layer', 'fsdp', None)
    in_specs = (dense_w, dense_w, dense_w, dense_f) * 4 + (stack_w, stack_w, stack_w, stack_f) * 2 + (stack_w, stack_w, stack_w, down_f)
    out_specs = (dense_w, dense_w, dense_f) * 4 + (stack_w, stack_w, stack_f) * 2 + (stack_w, stack_w, down_f)
    dma = pltpu.SemaphoreType.DMA
    anyspec = pl.BlockSpec(memory_space=pl.ANY)
    vspec = pl.BlockSpec(memory_space=pltpu.VMEM)

    def local_step(*blocks):
        mats = [blocks[4 * i:4 * i + 4] for i in range(7)]
        for i in (4, 5):
            mats[i] = tuple(jnp.swapaxes(a, 1, 2) for a in mats[i])
        mats[6] = mats[6][:3] + (jnp.swapaxes(mats[6][3], 1, 2),)
        first = []
        for x, m, g, q in mats:
            first += [m, g, q]
        scratch = [
            vm(ND, SQ, SQ), vm(ND, SQ, SQ, dtype=BF16), vm(ND, SQ, RD),
            vm(NG, SN, SQ), vm(NG, SN, SQ, dtype=BF16), vm(NG, RX, SN),
            vm(NE, SN, SQ), vm(NE, SN, SQ, dtype=BF16), vm(NE, RX, SN),
            vm(ND, 3, SQ, SQ, dtype=BF16), vm(NG, 3, SN, SQ, dtype=BF16), vm(NE, 3, SN, SQ, dtype=BF16)]
        scratch += [vm(ND, RD, SQ)] * 3 + [vm(NG, RE, SQ)] * 3 + [vm(NE, RE, SQ)] * 3
        for n, rp, w in ((ND, RD, SQ + 128), (NG, RE, 512), (NE, RE, 512)):
            scratch += [vm(n, rp, w), vm(n, rp // 2, w), vm(n, rp // 2, w), vm(n, rp, w)]
        for n, rp in ((ND, RD), (NG, RE), (NE, RE)):
            scratch += [vm(n, rp, 128), vm(n, rp, 128)]
        scratch += [vm(128, 128), vm(4, 16, 128), vm(128, 128), vm(4, 16, 128)]
        scratch += [dma((3, 13))]
        scratch += [dma((3, n)) for n in (2 * ND, 2 * ND, NG, NG, 2 * NE, 2 * NE, ND, ND, NG, NG, NE, NE)]
        scratch += [dma((4,))] * 4
        shapes = [(ND, RD, SQ), (NG, RE, SQ), (NE, RE, SQ), (ND, RD, SQ), (NG, RE, SN), (NE, RE, SN), (128, 128), (128, 128)]
        mids = pl.pallas_call(
            comm_kernel,
            out_shape=[jax.ShapeDtypeStruct(s, F32) for s in shapes],
            in_specs=[anyspec] * 21,
            out_specs=[vspec] * 8,
            scratch_shapes=scratch,
            name='comm',
            compiler_params=pltpu.CompilerParams(collective_id=0, has_side_effects=True, vmem_limit_bytes=VMEM_MAX),
        )(*first)
        second, shapes2, ospecs = [], [], []
        for x, m, g, q in mats:
            second += [x, m, g]
            shapes2 += [x, m, q]
            ospecs += [anyspec, anyspec, vspec]
        res = list(pl.pallas_call(
            update_kernel,
            out_shape=[jax.ShapeDtypeStruct(a.shape, F32) for a in shapes2],
            in_specs=[vspec] * 8 + [anyspec] * 21,
            out_specs=ospecs,
            scratch_shapes=[vm(ND, SQ, SQ), vm(ND, SQ, SQ), vm(ND, SQ, SQ, dtype=BF16),
                            vm(NG, SN, SQ), vm(NG, SN, SQ), vm(NG, SN, SQ, dtype=BF16),
                            vm(NE, SN, SQ), vm(NE, SN, SQ), vm(NE, SN, SQ, dtype=BF16), dma((3, 13)), dma((2, 13))],
            name='update',
            compiler_params=pltpu.CompilerParams(vmem_limit_bytes=VMEM_MAX),
        )(*mids, *second))
        for i in (12, 13, 14, 15, 16, 17, 20):
            res[i] = jnp.swapaxes(res[i], 1, 2)
        return tuple(res)

    return jax.shard_map(local_step, mesh=mesh, in_specs=in_specs, out_specs=out_specs, check_vma=False)
```

```python
import functools
import math
import jax
import jax.numpy as jnp
from jax import lax
from jax.experimental import pallas as pl
from jax.experimental.pallas import tpu as pltpu
from jax.sharding import PartitionSpec as P

MOMENTUM = 0.9
LEARN_RATE = 0.3
SLOTS = 4
RING = 4
COMM_VMEM = 26 * 1024 * 1024
UPDATE_VMEM = 16 * 1024 * 1024
TAGS = ('d0', 'd1', 'd2', 'd3', 'ga', 'up', 'dn')
F32 = jnp.float32
BF16 = jnp.bfloat16
ND, NG, NE = 4, 6, 3
RD, RE, RX = 128, 96, 88
SQ, SN = 512, 352

SCHEDULE = (
    'Pd0 Pd1 Pn0 Pn1', 'Pn2 y2n0 Pd2 y2n1', 'y2n2 Pd3 S0 Pg0', 'Pg1 Pg2 S1 Pg3', 'y3n0 Pg4 Pg5 y3n1', 'S2 T0 Qn0 Qn1',
    'y3n2 T1 S3 Qn2', 'T2 S4 Qd0 S5', 'T3 y2d0 T4 S6', 'S7 T5 Qd1 S8', 'S9 y2d1 S10 T6', 'y3d0 T7 Qd2 S11',
    'T8 T9 y2d2 T10', 'y3d1 S12 Qd3 T11', 'y2d3 S13 y3d2 Cn012', '@4 T12 @6 S14', 'end y3d3 Qg0 T13', 'pn0 Cd0123 @0 S15',
    'y2g0 @5 T14 @7', 'S16 @10 y3g0 @12', 'T15 S17 end Qg1', 'Qg2 S18 y2g1 T16', 'Qg3 y2g2 Od0 Od1', 'S19 y2g3 Qg4 T17',
    'Od2 Od3 y2g4 y3g1', 'pn1 pn2 T18 Qg5', 'y3g2 y2g5 T19 Cg012', '@0 y3g3 @5 y3g4', 'end y3g5 Og0 Og1',
    'Cg345 end Og2 Og3', 'Og4 Og5 rn0 rn1', 'rn2',
)


def split3(x):
    hi = x.astype(BF16)
    rest = x - hi.astype(F32)
    mid = rest.astype(BF16)
    low = (rest - mid.astype(F32)).astype(BF16)
    return hi, mid, low


def dot(a, b, trans=False):
    dims = (((1,), (1 if trans else 0,)), ((), ()))
    return lax.dot_general(a, b, dims, preferred_element_type=F32)


def mm6(a3, r, b1, b2, b3, trans=False):
    o1 = dot(a3, b1, trans)
    o2 = dot(a3[:2 * r], b2, trans)
    o3 = dot(a3[:r], b3, trans)
    return o1[:r] + ((o1[r:2 * r] + o2[:r]) + ((o1[2 * r:] + o2[r:]) + o3))


def stack3(x):
    return jnp.concatenate(split3(x), axis=0)


def load_split(b_ref, sp_ref, k, rows, g_ref=None, j=0):
    step = 32

    def body(c, carry):
        sl = pl.ds(pl.multiple_of(c * step, step), step)
        b = b_ref[k, sl, :]
        if g_ref is not None:
            b = b + g_ref[j, sl, :].astype(F32)
            b_ref[k, sl, :] = b
        for i, piece in enumerate(split3(b)):
            sp_ref[i, sl, :] = piece
        return carry

    lax.fori_loop(0, rows // step, body, 0)


def sub_bcast(x, t):
    return jnp.broadcast_to(x[t:t + 1, :], (8, 128))


def chol_step(a_ref, li_ref, ks, jb, rp):
    lane = lax.broadcasted_iota(jnp.int32, (8, 128), 1)
    sub = lax.broadcasted_iota(jnp.int32, (8, 128), 0)
    base = jb * 8
    row0 = pl.multiple_of(base, 8)
    n = range(len(ks))
    panel = [a_ref[k, pl.ds(row0, 8), :] for k in ks]
    idx = [jnp.full((8, 128), 0, jnp.int32) + (base + s) for s in range(8)]
    cols = [[jnp.take_along_axis(panel[i], idx[s], axis=1, mode='promise_in_bounds') for s in range(8)] for i in n]
    rinv = [jnp.zeros((8, 128), F32) for i in n]
    for t in range(8):
        inv = [1.0 / sub_bcast(cols[i][t], t) for i in n]
        for i in n:
            rinv[i] = jnp.where(sub == t, inv[i], rinv[i])
        mult = [jnp.where(sub > t, cols[i][t] * inv[i], 0.0) for i in n]
        for i in n:
            for s in range(8):
                if s != t:
                    cols[i][s] = cols[i][s] - mult[i] * sub_bcast(cols[i][s], t)
            cols[i][t] = jnp.where(sub == t, 1.0, -mult[i])
    low = [[jnp.where(sub >= s, cols[i][s], 0.0) for s in range(8)] for i in n]
    rows = []
    for i in n:
        r = low[i][0] * sub_bcast(panel[i], 0)
        for s in range(1, 8):
            r = r + low[i][s] * sub_bcast(panel[i], s)
        for s in range(8):
            r = jnp.where(lane == base + s, low[i][s], r)
        rows.append(r)
    upd = []
    for i in n:
        f = jnp.where(lane >= base + 8, rows[i] * rinv[i], 0.0)
        f1, f2, f3 = [x.astype(F32) for x in split3(f)]
        r1, r2, r3 = [x.astype(F32) for x in split3(rows[i])]
        lhs = jnp.concatenate([f1, f1, f2, f2, f1, f3], axis=0)
        rhs = jnp.concatenate([r1, r2, r1, r2, r3, r1], axis=0)
        upd.append(lax.dot_general(lhs.T, rhs, (((1,), (0,)), ((), ())), preferred_element_type=F32))
    lane_all = lax.broadcasted_iota(jnp.int32, (rp, 128), 1)
    inside = (lane_all >= base) & (lane_all < base + 8)
    for i in n:
        a_ref[ks[i]] = jnp.where(inside, 0.0, a_ref[ks[i]]) - upd[i][:rp]
    for i in n:
        li_ref[ks[i], pl.ds(row0, 8), :] = jnp.where(lane < base + 8, rows[i] * jnp.sqrt(rinv[i]), 0.0)


def chol(a_ref, li_ref, ks, nblk, rp, duties=()):
    def body(jb, carry):
        chol_step(a_ref, li_ref, ks, jb, rp)
        for at, duty in duties:
            pl.when(jb == at)(duty)
        return carry

    lax.fori_loop(0, nblk, body, 0)


def comm_kernel(*refs):
    names = []
    for t in TAGS:
        names += ['x' + t, 'm' + t, 'g' + t, 'q' + t]
    names += [
        'po_d', 'po_g', 'po_n', 'rt_d', 'rt_g', 'rt_n', 'inv_t', 'inv_f', 'Bd', 'Bg', 'Bn', 'Xd', 'Xg', 'Xn',
        'sp', 'Gd', 'Ge', 'Qd', 'Qg', 'Qn',
        'pd', 'pdT', 'pdB', 'pg', 'pgT', 'pgB', 'vn', 'vnT', 'vnB',
        'yd', 'yd1', 'yd2', 'ydT', 'yg', 'yg1', 'yg2', 'ygT', 'yn', 'yn1', 'yn2', 'ynT',
        'Ad', 'Ld', 'Ag', 'Lg', 'An', 'Ln', 'st', 'sr', 'ft', 'fr',
        'lsem', 'zs_d', 'zr_d', 'zs_g', 'zr_g', 'zs_n', 'zr_n', 'ys_d', 'yr_d', 'ys_g', 'yr_g', 'ys_n', 'yr_n',
        'ns', 'nr', 'fs', 'fr2']
    v = dict(zip(names, refs))
    assert len(names) == len(refs)
    z = lax.axis_index('tp')
    f = lax.axis_index('fsdp')
    core = lax.rem(f, 2)
    outer = (z == 0) | (z == 3)
    inner = jnp.logical_not(outer)
    edge = z + 1 - 2 * lax.rem(z, 2)
    mid = 3 - z
    core_p = f + 1 - 2 * core
    y_p = lax.rem(f + 2, 4)

    def lcopy(src, dst, i, j):
        return pltpu.make_async_copy(src, dst, v['lsem'].at[i, j])

    def source(c, g, k):
        if g == 'd':
            return v[c + TAGS[k]]
        if g == 'n':
            return v[c + 'dn'].at[k]
        return v[c + ('ga' if k < 3 else 'up')].at[k % 3]

    def load(c, g, k):
        i = {'d': 0, 'n': ND, 'g': ND + NE}[g] + k
        dst = v[('X' if c == 'x' else 'B') + g].at[k]
        if c == 'g':
            ref, j = place(g, k)
            dst = v[ref].at[j]
        if c == 'q':
            dst = v['Q' + g].at[k]
        return lcopy(source(c, g, k), dst, 'mgqx'.index(c), i)

    def place(g, k):
        if g == 'd':
            return 'Gd', k % 2
        return 'Ge', (k if g == 'n' else NE + k) % SLOTS

    def refill(g, k):
        if g == 'd':
            nxt = ('d', k + 2)
            ok = k + 2 < ND
        else:
            e = (k if g == 'n' else NE + k) + SLOTS
            ok = e < NE + NG
            nxt = ('g', e - NE)
        if ok:
            load('g', *nxt).start()

    order = [('d', k) for k in range(ND)] + [('n', k) for k in range(NE)] + [('g', k) for k in range(NG)]
    for g, k in order:
        for c in 'mgq':
            if c != 'g' or (k < 2 if g == 'd' else (g == 'n' or NE + k < SLOTS)):
                load(c, g, k).start()

    barrier = pltpu.get_barrier_semaphore()
    for d in range(1, 4):
        pl.semaphore_signal(barrier, inc=1, device_id={'tp': lax.rem(z + d, 4)}, device_id_type=pl.DeviceIdType.MESH)
        pl.semaphore_signal(barrier, inc=1, device_id={'fsdp': lax.rem(f + d, 4)}, device_id_type=pl.DeviceIdType.MESH)
    pl.semaphore_wait(barrier, 6)

    def remote(src, dst, ssem, rsem, dev):
        return pltpu.make_async_remote_copy(src_ref=src, dst_ref=dst, send_sem=ssem, recv_sem=rsem,
                                            device_id=dev, device_id_type=pl.DeviceIdType.MESH)

    def zpiece(own, t, b, ss, rs, i, k, row0, rows, col0, cols):
        own, t, b = [v[x].at[k, pl.ds(row0, rows), pl.ds(col0, cols)] for x in (own, t, b)]
        ss, rs = v[ss], v[rs]
        def ca():
            return remote(own, t, ss.at[0, i], rs.at[0, i], {'tp': edge})
        def cb():
            return remote(own, b, ss.at[1, i], rs.at[1, i], {'tp': mid})
        def ct():
            return remote(t, t, ss.at[2, i], rs.at[2, i], {'tp': edge})

        def send():
            @pl.when(outer)
            def _():
                ca().start()

        def half():
            @pl.when(inner)
            def _():
                ca().wait_recv()
                own[...] = own[...] + t[...]
                cb().start()

        def total():
            @pl.when(inner)
            def _():
                cb().wait_recv()
                t[...] = own[...] + b[...]
                ct().start()

        def take():
            @pl.when(outer)
            def _():
                ct().wait_recv()

        def done():
            @pl.when(outer)
            def _():
                ca().wait_send()

            @pl.when(inner)
            def _():
                cb().wait_send()
                ct().wait_send()

        return send, half, total, take, done

    def yset(own, r1, r2, t, ss, rs, half):
        own, r1, r2, t, ss, rs = v[own], v[r1], v[r2], v[t], v[ss], v[rs]
        h = r1
        mine = pl.ds(pl.multiple_of(core * half, 8), half)
        theirs = pl.ds(pl.multiple_of((1 - core) * half, 8), half)

        def c1(k):
            return remote(own.at[k, theirs, :], r1.at[k], ss.at[0, k], rs.at[0, k], {'fsdp': core_p})

        def c2(k):
            return remote(h.at[k], r2.at[k], ss.at[1, k], rs.at[1, k], {'fsdp': y_p})

        def c3(k):
            return remote(t.at[k, mine, :], t.at[k, mine, :], ss.at[2, k], rs.at[2, k], {'fsdp': core_p})

        def y1(k):
            c1(k).start()

        def y2(k):
            c1(k).wait_recv()
            h[k] = own[k, mine, :] + r1[k]
            c2(k).start()

        def y3(k):
            c2(k).wait_recv()
            t[k, mine, :] = h[k] + r2[k]
            c3(k).start()

        def y4(k):
            remote(t.at[k, mine, :], t.at[k, theirs, :], ss.at[2, k], rs.at[2, k], {'fsdp': core_p}).wait_recv()

        def fin(k):
            c1(k).wait_send()
            c2(k).wait_send()
            c3(k).wait_send()

        return y1, y2, y3, y4, fin

    Z = []
    where = {}
    for k in range(ND):
        for h in range(2):
            where['d', k, h] = len(Z)
            Z.append(zpiece('pd', 'pdT', 'pdB', 'zs_d', 'zr_d', 2 * k + h, k, h * 64, 64, 0, SQ))
    for k in range(NE):
        where['G', k] = len(Z)
        Z.append(zpiece('vn', 'vnT', 'vnB', 'zs_n', 'zr_n', k, k, 0, RX, 384, 128))
    for k in range(NG):
        where['g', k] = len(Z)
        Z.append(zpiece('pg', 'pgT', 'pgB', 'zs_g', 'zr_g', k, k, 0, RX, 0, SQ))
    for k in range(NE):
        where['Y', k] = len(Z)
        Z.append(zpiece('vn', 'vnT', 'vnB', 'zs_n', 'zr_n', NE + k, k, 0, RX, 0, 384))


    keys = sorted(where, key=where.get)

    def S(n):
        Z[n][1]()

    def T(n):
        Z[n][2]()

    def W(*key):
        Z[where[key]][3]()

    yd = yset('yd', 'yd1', 'yd2', 'ydT', 'ys_d', 'yr_d', RD // 2)
    yg = yset('yg', 'yg1', 'yg2', 'ygT', 'ys_g', 'yr_g', RE // 2)
    yn = yset('yn', 'yn1', 'yn2', 'ynT', 'ys_n', 'yr_n', RE // 2)

    def loop(n, body):
        def go(k, carry):
            body(k)
            return carry
        lax.fori_loop(0, n, go, 0)

    zero_rows = jnp.zeros((RE - RX, SQ), F32)

    def q_stack(qt, rp):
        if rp != qt.shape[0]:
            qt = jnp.concatenate([qt, jnp.zeros((rp - qt.shape[0], qt.shape[1]), F32)], axis=0)
        return stack3(qt)

    def pieces(g):
        rows = v['B' + g].shape[1]
        return [v['sp'][i, :rows] for i in range(3)]

    def part(g, k):
        for c in 'mgq':
            load(c, g, k).wait()
        ref, j = place(g, k)
        load_split(v['B' + g], v['sp'], k, v['B' + g].shape[1], v[ref], j)
        refill(g, k)
        load('x', g, k).start()
        q = v['Q' + g][k]
        own, trans = {'d': ('pd', True), 'g': ('pg', False), 'n': ('yn', False)}[g]
        rp = RD if g == 'd' else RE
        v[own][k] = mm6(q_stack(q.T if g == 'd' else q, rp), rp, *pieces(g), trans)
        if g == 'g':
            v['pgT'][k, RX:] = zero_rows
        if g == 'n':
            yn[0](k)

    def gram(p3, rp):
        return mm6(p3, rp, p3[:rp], p3[rp:2 * rp], p3[2 * rp:], True)

    def post_d(k):
        W('d', k, 0)
        W('d', k, 1)
        p3 = stack3(v['pdT'][k])
        load_split(v['Bd'], v['sp'], k, v['Bd'].shape[1])
        v['yd'][k, :, :SQ] = mm6(p3, RD, *pieces('d'))
        v['yd'][k, :, SQ:] = gram(p3, RD)
        yd[0](k)

    def post_g(k):
        W('g', k)
        p3 = stack3(v['pgT'][k])
        load_split(v['Bg'], v['sp'], k, v['Bg'].shape[1])
        v['yg'][k, :, :SN] = mm6(p3, RE, *pieces('g'), True)
        v['yg'][k, :, SN:384] = jnp.zeros((RE, 384 - SN), F32)
        v['yg'][k, :, 384:384 + RE] = gram(p3, RE)
        v['yg'][k, :, 384 + RE:] = jnp.zeros((RE, 128 - RE), F32)
        yg[0](k)

    def post_n(k):
        yn[3](k)
        p3 = stack3(v['ynT'][k])
        load_split(v['Bn'], v['sp'], k, v['Bn'].shape[1])
        v['vn'][k, :, :SN] = mm6(p3, RE, *pieces('n'), True)
        v['vn'][k, :, SN:384] = jnp.zeros((RE, 384 - SN), F32)
        v['vn'][k, :, 384:384 + RE] = gram(p3, RE)
        v['vn'][k, :, 384 + RE:] = jnp.zeros((RE, 128 - RE), F32)
        v['vnT'][k, RX:] = zero_rows

    def orth_p(l_ref, p_ref, po, k, rp):
        l3 = stack3(l_ref[k, :, :rp])
        q3 = stack3(p_ref[k])
        po[k] = mm6(l3, rp, q3[:rp], q3[rp:2 * rp], q3[2 * rp:])

    def orth_r(l_ref, y_ref, rt, k, rp, width, norm, lane):
        l3 = stack3(l_ref[k, :, :rp])
        y3 = stack3(y_ref[k, :, :width])
        res = mm6(l3, rp, y3[:rp], y3[rp:2 * rp], y3[2 * rp:])
        rt[k] = res
        col = jnp.sum(res * res, axis=1, keepdims=True)
        here = lax.broadcasted_iota(jnp.int32, (rp, 128), 1) == lane
        norm[:rp] = jnp.where(here, jnp.broadcast_to(col, (rp, 128)), norm[:rp])

    def orth_d(k):
        orth_p(v['Ld'], v['pdT'], v['po_d'], k, RD)
        orth_r(v['Ld'], v['ydT'], v['rt_d'], k, RD, SQ, v['st'], k)

    def orth_g(k):
        orth_p(v['Lg'], v['pgT'], v['po_g'], k, RE)
        orth_r(v['Lg'], v['ygT'], v['rt_g'], k, RE, SN, v['st'], ND + k)

    def take_d(k):
        yd[3](k)
        v['Ad'][k] = v['ydT'][k, :, SQ:]

    def take_g(k):
        yg[3](k)
        v['Ag'][k] = v['ygT'][k, :, 384:]
        v['Lg'][k, RX:] = jnp.zeros((RE - RX, 128), F32)

    def take_n(k):
        W('G', k)
        v['An'][k] = v['vnT'][k, :, 384:]
        v['Ln'][k, RX:] = jnp.zeros((RE - RX, 128), F32)

    v['st'][...] = jnp.zeros((128, 128), F32)
    v['ft'][...] = jnp.zeros((128, 128), F32)


    made, sent = set(), [0]

    def ship():
        while sent[0] < len(Z) and keys[sent[0]][:2] in made:
            Z[sent[0]][0]()
            sent[0] += 1

    def last_r(k):
        W('Y', k)
        orth_r(v['Ln'], v['vnT'], v['rt_n'], k, RE, SN, v['ft'], k)

    table = {'Pd': functools.partial(part, 'd'), 'Pn': functools.partial(part, 'n'), 'Pg': functools.partial(part, 'g'), 'Qd': post_d, 'Qn': post_n, 'Qg': post_g, 'Od': orth_d, 'Og': orth_g,
             'pn': lambda k: orth_p(v['Ln'], v['ynT'], v['po_n'], k, RE), 'rn': last_r}
    groups = {'d': ('Ad', 'Ld', RD, RD, take_d, yd), 'g': ('Ag', 'Lg', RX, RE, take_g, yg), 'n': ('An', 'Ln', RX, RE, take_n, yn)}

    def do(word):
        if word[0] == 'S':
            S(int(word[1:]))
        elif word[0] == 'T':
            T(int(word[1:]))
        elif word[0] == 'y':
            groups[word[2]][5][int(word[1]) - 1](int(word[3]))
        else:
            k = int(word[2])
            table[word[:2]](k)
            if word[:2] in ('Pd', 'Pg'):
                made.add((word[1], k))
            if word[:2] == 'Qn':
                made.update((('G', k), ('Y', k)))
            ship()

    words = [w for line in SCHEDULE for w in line.split()]
    while words:
        word = words.pop(0)
        if word[0] != 'C':
            do(word)
            continue
        a, l, r, rp, take, _ = groups[word[1]]
        ks = [int(c) for c in word[2:]]
        duties = []
        while words[0] != 'end':
            w = words.pop(0)
            if w[0] == '@':
                duties.append((int(w[1:]), []))
            else:
                duties[-1][1].append(w)
        words.pop(0)
        for k in ks:
            take(k)
        chol(v[a], v[l], ks, r // 8, rp, [(at, functools.partial(lambda todo: [do(w) for w in todo] and None, todo)) for at, todo in duties])

    v['sr'][0] = v['st'][...].T[:16]
    v['fr'][0] = v['ft'][...].T[:16]
    copies = []
    for d in range(1, 4):
        copies.append(remote(v['sr'].at[0], v['sr'].at[d], v['ns'].at[d], v['nr'].at[d], {'tp': lax.rem(z + d, 4)}))
        copies.append(remote(v['fr'].at[0], v['fr'].at[d], v['fs'].at[d], v['fr2'].at[d], {'fsdp': lax.rem(f + d, 4)}))
    for c in copies:
        c.start()
    for c in copies:
        c.wait_recv()
    pad = jnp.zeros((112, 128), F32)
    tot_t = (v['sr'][0] + v['sr'][2]) + (v['sr'][1] + v['sr'][3])
    tot_f = (v['fr'][0] + v['fr'][2]) + (v['fr'][1] + v['fr'][3])
    inv_t = jnp.where(tot_t > 0.0, 1.0 / jnp.sqrt(tot_t), 0.0)
    inv_f = jnp.where(tot_f > 0.0, 1.0 / jnp.sqrt(tot_f), 0.0)
    v['inv_t'][...] = jnp.concatenate([inv_t, pad], axis=0).T
    v['inv_f'][...] = jnp.concatenate([inv_f, pad], axis=0).T

    for c in copies:
        c.wait_send()
    for piece in Z:
        piece[4]()
    for g, k in order:
        load('x', g, k).wait()
    loop(ND, yd[4])
    loop(NG, yg[4])
    loop(NE, yn[4])


def update_kernel(*refs):
    names = ['po_d', 'po_g', 'po_n', 'rt_d', 'rt_g', 'rt_n', 'inv_t', 'inv_f', 'Bd', 'Bg', 'Bn', 'Xd', 'Xg', 'Xn']
    for t in TAGS:
        names += ['X' + t, 'M' + t, 'Q' + t]
    names += ['ms', 'xs', 'qd', 'qg', 'qn', 'osem']
    v = dict(zip(names, refs))
    assert len(names) == len(refs)
    tags = [(t, None) for t in TAGS[:4]] + [(t, e) for t in TAGS[4:] for e in range(3)]

    def at(name, e):
        return v[name] if e is None else v[name].at[e]

    def slot(i):
        if i < 4:
            return 'd', i
        if i < 10:
            return 'g', i - 4
        return 'n', i - 10

    stores = []
    for i, (tag, e) in enumerate(tags):
        g, k = slot(i)
        rows = v['B' + g].shape[1]
        stores.append([pltpu.make_async_copy(v['ms'].at[i % RING, :rows], at('M' + tag, e), v['osem'].at[0, i]),
                       pltpu.make_async_copy(v['xs'].at[i % RING, :rows], at('X' + tag, e), v['osem'].at[1, i]),
                       pltpu.make_async_copy(v['q' + g].at[k], at('Q' + tag, e), v['osem'].at[2, i])])

    def pack(x):
        a, b, c = split3(x)
        return jnp.concatenate([a, b], axis=1), jnp.concatenate([a, c], axis=1)

    def packs(y):
        a, b, c = split3(y)
        return (jnp.concatenate([a, b], axis=0), jnp.concatenate([b, a], axis=0), jnp.concatenate([c, a], axis=0))

    def pad(x):
        if x.shape[0] == 128:
            return x
        return jnp.concatenate([x, jnp.zeros((128 - x.shape[0], x.shape[1]), F32)], axis=0)

    def prod(lhs, rhs):
        return dot(lhs[0], rhs[0]) + (dot(lhs[0], rhs[1]) + dot(lhs[1], rhs[2]))

    for i, (tag, e) in enumerate(tags):
        g, k = slot(i)
        pt = pad(v['po_' + g][k])
        rt = pad(v['rt_' + g][k])
        inv = v['inv_f'][:, k:k + 1] if g == 'n' else v['inv_t'][:, i:i + 1]
        qt = rt * jnp.broadcast_to(inv, rt.shape)
        flip = g != 'd'
        q = qt[:RX] if flip else qt.T
        v['q' + g][k] = q
        stores[i][2].start()
        eta = LEARN_RATE * (math.sqrt(2048 / 1408) if flip else 1.0)
        if flip:
            rhs = packs(pt)
            lhs_m, rhs_m, lhs_x, rhs_x = pack(rt.T), rhs, pack(qt.T), rhs
        else:
            lhs = pack(pt.T)
            lhs_m, rhs_m, lhs_x, rhs_x = lhs, packs(rt), lhs, packs(qt)
        rows = v['B' + g].shape[1]
        if i >= RING:
            stores[i - RING][0].wait()
            stores[i - RING][1].wait()
        v['ms'][i % RING, :rows] = v['B' + g][k] - (1.0 - MOMENTUM) * prod(lhs_m, rhs_m)
        stores[i][0].start()
        v['xs'][i % RING, :rows] = v['X' + g][k] - eta * prod(lhs_x, rhs_x)
        stores[i][1].start()
    for i, group in enumerate(stores):
        for c in group[2:] if i < len(stores) - RING else group:
            c.wait()


def vm(*shape, dtype=F32):
    return pltpu.VMEM(shape, dtype)


def solution(mesh):
    dense_w = P(('layer', 'fsdp'), 'tp')
    dense_f = P(('layer', 'tp'), None)
    stack_w = P('layer', 'fsdp', 'tp')
    stack_f = P('layer', 'tp', None)
    down_f = P('layer', 'fsdp', None)
    in_specs = (dense_w, dense_w, dense_w, dense_f) * 4 + (stack_w, stack_w, stack_w, stack_f) * 2 + (stack_w, stack_w, stack_w, down_f)
    out_specs = (dense_w, dense_w, dense_f) * 4 + (stack_w, stack_w, stack_f) * 2 + (stack_w, stack_w, down_f)
    dma = pltpu.SemaphoreType.DMA
    hbm = pl.BlockSpec(memory_space=pltpu.HBM)
    vspec = pl.BlockSpec(memory_space=pltpu.VMEM)

    def local_step(*blocks):
        mats = [blocks[4 * i:4 * i + 4] for i in range(7)]
        for i in (4, 5):
            mats[i] = tuple(jnp.swapaxes(a, 1, 2) for a in mats[i])
        mats[6] = mats[6][:3] + (jnp.swapaxes(mats[6][3], 1, 2),)
        scratch = [vm(3, SQ, SQ, dtype=BF16), vm(2, SQ, SQ, dtype=BF16), vm(SLOTS, SN, SQ, dtype=BF16), vm(ND, SQ, RD), vm(NG, RX, SN), vm(NE, RX, SN)]
        scratch += [vm(ND, RD, SQ)] * 3 + [vm(NG, RE, SQ)] * 3 + [vm(NE, RE, SQ)] * 3
        for n, rp, w in ((ND, RD, SQ + 128), (NG, RE, 512), (NE, RE, 512)):
            scratch += [vm(n, rp, w), vm(n, rp // 2, w), vm(n, rp // 2, w), vm(n, rp, w)]
        for n, rp in ((ND, RD), (NG, RE), (NE, RE)):
            scratch += [vm(n, rp, 128), vm(n, rp, 128)]
        scratch += [vm(128, 128), vm(4, 16, 128), vm(128, 128), vm(4, 16, 128)]
        scratch += [dma((4, 13))]
        scratch += [dma((3, n)) for n in (2 * ND, 2 * ND, NG, NG, 2 * NE, 2 * NE, ND, ND, NG, NG, NE, NE)]
        scratch += [dma((4,))] * 4
        shapes = [(ND, RD, SQ), (NG, RE, SQ), (NE, RE, SQ), (ND, RD, SQ), (NG, RE, SN), (NE, RE, SN), (128, 128), (128, 128),
                  (ND, SQ, SQ), (NG, SN, SQ), (NE, SN, SQ), (ND, SQ, SQ), (NG, SN, SQ), (NE, SN, SQ)]
        mids = pl.pallas_call(
            comm_kernel,
            out_shape=[jax.ShapeDtypeStruct(s, F32) for s in shapes],
            in_specs=[hbm] * 28,
            out_specs=[vspec] * 14,
            scratch_shapes=scratch,
            name='comm',
            compiler_params=pltpu.CompilerParams(collective_id=0, has_side_effects=True, vmem_limit_bytes=COMM_VMEM),
        )(*[pltpu.with_memory_space_constraint(a, pltpu.HBM) for m in mats for a in m])
        res = list(pl.pallas_call(
            update_kernel,
            out_shape=[jax.ShapeDtypeStruct(m[j].shape, F32) for m in mats for j in (0, 1, 3)],
            in_specs=[vspec] * 14,
            out_specs=[hbm] * 21,
            scratch_shapes=[vm(RING, SQ, SQ), vm(RING, SQ, SQ), vm(ND, SQ, RD), vm(NG, RX, SN), vm(NE, RX, SN), dma((3, 13))],
            name='update',
            compiler_params=pltpu.CompilerParams(vmem_limit_bytes=UPDATE_VMEM),
        )(*mids))
        for i in (12, 13, 14, 15, 16, 17, 20):
            res[i] = jnp.swapaxes(res[i], 1, 2)
        return tuple(res)

    return jax.shard_map(local_step, mesh=mesh, in_specs=in_specs, out_specs=out_specs, check_vma=False)
```

```python
import functools
import math
import jax
import jax.numpy as jnp
from jax import lax
from jax.experimental import pallas as pl
from jax.experimental.pallas import tpu as pltpu
from jax.sharding import PartitionSpec as P

MOMENTUM = 0.9
LEARN_RATE = 0.3
SLOTS = 4
RING = 4
COMM_VMEM = 26 * 1024 * 1024
UPDATE_VMEM = 16 * 1024 * 1024
TAGS = ('d0', 'd1', 'd2', 'd3', 'ga', 'up', 'dn')
F32 = jnp.float32
BF16 = jnp.bfloat16
ND, NG, NE = 4, 6, 3
RD, RE, RX = 128, 96, 88
SQ, SN = 512, 352
DENSE_ITEMS = ((0, 0, 32), (0, 32, 32), (0, 64, 64)) + tuple((k, h, 64) for k in range(1, ND) for h in (0, 64))

SCHEDULE = ''.join((
    'iikkkkSkiSkjjSTjciTccSTShmSThmTShlmTSaTSlSSTaSeSTlSTTaTSeTSl',
    'TSaCn3@ASTe@DT@ES@ISTEoSTeuuoSTbCd4@BTbS@ETS@HT@If@KS@LT@Mf@',
    'OTESoobTSobqqqboTqsbfsvTCg3@Bf@GfErfrrvvCg3ErrrZssutttttt',
))


def split3(x):
    hi = x.astype(BF16)
    rest = x - hi.astype(F32)
    mid = rest.astype(BF16)
    low = (rest - mid.astype(F32)).astype(BF16)
    return hi, mid, low


def dot(a, b, trans=False):
    dims = (((1,), (1 if trans else 0,)), ((), ()))
    return lax.dot_general(a, b, dims, preferred_element_type=F32)


def mm6(a3, r, b1, b2, b3, trans=False):
    o1 = dot(a3, b1, trans)
    o2 = dot(a3[:2 * r], b2, trans)
    o3 = dot(a3[:r], b3, trans)
    return o1[:r] + ((o1[r:2 * r] + o2[:r]) + ((o1[2 * r:] + o2[r:]) + o3))


def stack3(x):
    return jnp.concatenate(split3(x), axis=0)


def load_split(b_ref, sp_ref, k, rows, g_ref=None, j=0):
    step = 32

    def body(c, carry):
        sl = pl.ds(pl.multiple_of(c * step, step), step)
        b = b_ref[k, sl, :]
        if g_ref is not None:
            b = b + g_ref[j, sl, :].astype(F32)
            b_ref[k, sl, :] = b
        for i, piece in enumerate(split3(b)):
            sp_ref[i, sl, :] = piece
        return carry

    lax.fori_loop(0, rows // step, body, 0)


def sub_bcast(x, t):
    return jnp.broadcast_to(x[t:t + 1, :], (8, 128))


def chol_step(a_ref, li_ref, ks, jb, rp):
    lane = lax.broadcasted_iota(jnp.int32, (8, 128), 1)
    sub = lax.broadcasted_iota(jnp.int32, (8, 128), 0)
    base = jb * 8
    row0 = pl.multiple_of(base, 8)
    n = range(len(ks))
    panel = [a_ref[k, pl.ds(row0, 8), :] for k in ks]
    idx = [jnp.full((8, 128), 0, jnp.int32) + (base + s) for s in range(8)]
    cols = [[jnp.take_along_axis(panel[i], idx[s], axis=1, mode='promise_in_bounds') for s in range(8)] for i in n]
    rinv = [jnp.zeros((8, 128), F32) for i in n]
    for t in range(8):
        inv = [1.0 / sub_bcast(cols[i][t], t) for i in n]
        for i in n:
            rinv[i] = jnp.where(sub == t, inv[i], rinv[i])
        mult = [jnp.where(sub > t, cols[i][t] * inv[i], 0.0) for i in n]
        for i in n:
            for s in range(8):
                if s != t:
                    cols[i][s] = cols[i][s] - mult[i] * sub_bcast(cols[i][s], t)
            cols[i][t] = jnp.where(sub == t, 1.0, -mult[i])
    low = [[jnp.where(sub >= s, cols[i][s], 0.0) for s in range(8)] for i in n]
    rows = []
    for i in n:
        r = low[i][0] * sub_bcast(panel[i], 0)
        for s in range(1, 8):
            r = r + low[i][s] * sub_bcast(panel[i], s)
        for s in range(8):
            r = jnp.where(lane == base + s, low[i][s], r)
        rows.append(r)
    upd = []
    for i in n:
        f = jnp.where(lane >= base + 8, rows[i] * rinv[i], 0.0)
        f1, f2, f3 = [x.astype(F32) for x in split3(f)]
        r1, r2, r3 = [x.astype(F32) for x in split3(rows[i])]
        lhs = jnp.concatenate([f1, f1, f2, f2, f1, f3], axis=0)
        rhs = jnp.concatenate([r1, r2, r1, r2, r3, r1], axis=0)
        upd.append(lax.dot_general(lhs.T, rhs, (((1,), (0,)), ((), ())), preferred_element_type=F32))
    lane_all = lax.broadcasted_iota(jnp.int32, (rp, 128), 1)
    inside = (lane_all >= base) & (lane_all < base + 8)
    for i in n:
        a_ref[ks[i]] = jnp.where(inside, 0.0, a_ref[ks[i]]) - upd[i][:rp]
    for i in n:
        li_ref[ks[i], pl.ds(row0, 8), :] = jnp.where(lane < base + 8, rows[i] * jnp.sqrt(rinv[i]), 0.0)


def chol(a_ref, li_ref, ks, nblk, rp, duties=()):
    def body(jb, carry):
        chol_step(a_ref, li_ref, ks, jb, rp)
        for at, duty in duties:
            pl.when(jb == at)(duty)
        return carry

    lax.fori_loop(0, nblk, body, 0)


def comm_kernel(*refs):
    names = []
    for t in TAGS:
        names += ['x' + t, 'm' + t, 'g' + t, 'q' + t]
    names += [
        'po_d', 'po_g', 'po_n', 'rt_d', 'rt_g', 'rt_n', 'inv_t', 'inv_f', 'Bd', 'Bg', 'Bn', 'Xd', 'Xg', 'Xn',
        'sp', 'Gd', 'Ge', 'Qd', 'Qg', 'Qn',
        *[g + c for g in ('pd', 'pg', 'vn') for c in ('', 'T', 'B')],
        *[c for g in 'dgn' for c in ('y' + g, g + '1', g + '2', 'y' + g + 'T')],
        'Ad', 'Ld', 'Ag', 'Lg', 'An', 'Ln', 'st', 'sr', 'ft', 'fr',
        'lsem', *[a + g for a in 'zy' for g in ('s_d', 'r_d', 's_g', 'r_g', 's_n', 'r_n')],
        'ns', 'nr', 'fs', 'fr2']
    v = dict(zip(names, refs))
    assert len(names) == len(refs)
    z = lax.axis_index('tp')
    f = lax.axis_index('fsdp')
    core = lax.rem(f, 2)
    outer = (z == 0) | (z == 3)
    inner = jnp.logical_not(outer)
    edge = z + 1 - 2 * lax.rem(z, 2)
    mid = 3 - z
    core_p = f + 1 - 2 * core
    y_p = lax.rem(f + 2, 4)

    def lcopy(src, dst, i, j):
        return pltpu.make_async_copy(src, dst, v['lsem'].at[i, j])

    def source(c, g, k):
        if g == 'd':
            return v[c + TAGS[k]]
        if g == 'n':
            return v[c + 'dn'].at[k]
        return v[c + ('ga' if k < 3 else 'up')].at[k % 3]

    def load(c, g, k):
        i = {'d': 0, 'n': ND, 'g': ND + NE}[g] + k
        dst = v[('X' if c == 'x' else 'B') + g].at[k]
        if c == 'g':
            ref, j = place(g, k)
            dst = v[ref].at[j]
        if c == 'q':
            dst = v['Q' + g].at[k]
        return lcopy(source(c, g, k), dst, 'mgqx'.index(c), i)

    order = []
    for c in SCHEDULE:
        if c in 'ijk':
            g = 'dng'['ijk'.index(c)]
            order.append((g, sum(o[0] == g for o in order)))
    dense = [o for o in order if o[0] == 'd']
    experts = [o for o in order if o[0] != 'd']

    def place(g, k):
        if g == 'd':
            return 'Gd', k % 2
        return 'Ge', experts.index((g, k)) % SLOTS

    def refill(g, k):
        line, slots = (dense, 2) if g == 'd' else (experts, SLOTS)
        rest = line[line.index((g, k)) + slots:]
        if rest:
            load('g', *rest[0]).start()

    for o in order:
        for c in 'mgq':
            if c != 'g' or o in dense[:2] or o in experts[:SLOTS]:
                load(c, *o).start()

    barrier = pltpu.get_barrier_semaphore()
    for d in range(1, 4):
        pl.semaphore_signal(barrier, inc=1, device_id={'tp': lax.rem(z + d, 4)}, device_id_type=pl.DeviceIdType.MESH)
        pl.semaphore_signal(barrier, inc=1, device_id={'fsdp': lax.rem(f + d, 4)}, device_id_type=pl.DeviceIdType.MESH)
    pl.semaphore_wait(barrier, 6)

    def remote(src, dst, ssem, rsem, dev):
        return pltpu.make_async_remote_copy(src_ref=src, dst_ref=dst, send_sem=ssem, recv_sem=rsem,
                                            device_id=dev, device_id_type=pl.DeviceIdType.MESH)

    def zpiece(own, t, b, ss, rs, i, k, row0, rows, col0, cols):
        own, t, b = [v[x].at[k, pl.ds(row0, rows), pl.ds(col0, cols)] for x in (own, t, b)]
        ss, rs = v[ss], v[rs]
        def ca():
            return remote(own, t, ss.at[0, i], rs.at[0, i], {'tp': edge})
        def cb():
            return remote(own, b, ss.at[1, i], rs.at[1, i], {'tp': mid})
        def ct():
            return remote(t, t, ss.at[2, i], rs.at[2, i], {'tp': edge})

        def send():
            @pl.when(outer)
            def _():
                ca().start()

        def half():
            @pl.when(inner)
            def _():
                ca().wait_recv()
                own[...] = own[...] + t[...]
                cb().start()

        def total():
            @pl.when(inner)
            def _():
                cb().wait_recv()
                t[...] = own[...] + b[...]
                ct().start()

        def take():
            @pl.when(outer)
            def _():
                ct().wait_recv()

        def done():
            @pl.when(outer)
            def _():
                ca().wait_send()

            @pl.when(inner)
            def _():
                cb().wait_send()
                ct().wait_send()

        return send, half, total, take, done

    def yset(g, half):
        own, r1, r2, t, ss, rs = [v[c] for c in ('y' + g, g + '1', g + '2', 'y' + g + 'T', 'ys_' + g, 'yr_' + g)]
        h = r1
        mine = pl.ds(pl.multiple_of(core * half, 8), half)
        theirs = pl.ds(pl.multiple_of((1 - core) * half, 8), half)

        def c1(k):
            return remote(own.at[k, theirs, :], r1.at[k], ss.at[0, k], rs.at[0, k], {'fsdp': core_p})

        def c2(k):
            return remote(h.at[k], r2.at[k], ss.at[1, k], rs.at[1, k], {'fsdp': y_p})

        def c3(k):
            return remote(t.at[k, mine, :], t.at[k, mine, :], ss.at[2, k], rs.at[2, k], {'fsdp': core_p})

        def y1(k):
            c1(k).start()

        def y2(k):
            c1(k).wait_recv()
            h[k] = own[k, mine, :] + r1[k]
            c2(k).start()

        def y3(k):
            c2(k).wait_recv()
            t[k, mine, :] = h[k] + r2[k]
            c3(k).start()

        def y4(k):
            remote(t.at[k, mine, :], t.at[k, theirs, :], ss.at[2, k], rs.at[2, k], {'fsdp': core_p}).wait_recv()

        def fin(k):
            c1(k).wait_send()
            c2(k).wait_send()
            c3(k).wait_send()

        return y1, y2, y3, y4, fin

    Z, keys = [], []

    def line(kind, k, own, sems, i, row0, rows, col0, cols):
        keys.append((kind, k))
        Z.append(zpiece(own, own + 'T', own + 'B', 'zs_' + sems, 'zr_' + sems, i, k, row0, rows, col0, cols))

    for i, (k, row0, rows) in enumerate(DENSE_ITEMS):
        line('d', k, 'pd', 'd', i, row0, rows, 0, SQ)
    for k in range(NE):
        line('G', k, 'vn', 'n', k, 0, RX, 384, 128)
    for k in range(NG):
        line('g', k, 'pg', 'g', 2 * k, 0, 48, 0, SQ)
        line('g', k, 'pg', 'g', 2 * k + 1, 48, RX - 48, 0, SQ)
    for k in range(NE):
        line('Y', k, 'vn', 'n', NE + k, 0, RX, 0, 384)

    def S(n):
        Z[n][1]()

    def T(n):
        Z[n][2]()

    def W(kind, k):
        for key, piece in zip(keys, Z):
            if key == (kind, k):
                piece[3]()

    yd = yset('d', RD // 2)
    yg = yset('g', RE // 2)
    yn = yset('n', RE // 2)

    def loop(n, body):
        def go(k, carry):
            body(k)
            return carry
        lax.fori_loop(0, n, go, 0)

    zero_rows = jnp.zeros((RE - RX, SQ), F32)

    def q_stack(qt, rp):
        if rp != qt.shape[0]:
            qt = jnp.concatenate([qt, jnp.zeros((rp - qt.shape[0], qt.shape[1]), F32)], axis=0)
        return stack3(qt)

    def pieces(g):
        rows = v['B' + g].shape[1]
        return [v['sp'][i, :rows] for i in range(3)]

    def part(g, k):
        for c in 'mgq':
            load(c, g, k).wait()
        ref, j = place(g, k)
        load_split(v['B' + g], v['sp'], k, v['B' + g].shape[1], v[ref], j)
        refill(g, k)
        load('x', g, k).start()
        q = v['Q' + g][k]
        own, trans = {'d': ('pd', True), 'g': ('pg', False), 'n': ('yn', False)}[g]
        rp = RD if g == 'd' else RE
        v[own][k] = mm6(q_stack(q.T if g == 'd' else q, rp), rp, *pieces(g), trans)
        if g == 'g':
            v['pgT'][k, RX:] = zero_rows
        if g == 'n':
            yn[0](k)

    def gram(p3, rp):
        return mm6(p3, rp, p3[:rp], p3[rp:2 * rp], p3[2 * rp:], True)

    def post_d(k):
        W('d', k)
        p3 = stack3(v['pdT'][k])
        load_split(v['Bd'], v['sp'], k, v['Bd'].shape[1])
        v['yd'][k, :, :SQ] = mm6(p3, RD, *pieces('d'))
        v['yd'][k, :, SQ:] = gram(p3, RD)
        yd[0](k)

    def post_g(k):
        W('g', k)
        p3 = stack3(v['pgT'][k])
        load_split(v['Bg'], v['sp'], k, v['Bg'].shape[1])
        v['yg'][k, :, :SN] = mm6(p3, RE, *pieces('g'), True)
        v['yg'][k, :, SN:384] = jnp.zeros((RE, 384 - SN), F32)
        v['yg'][k, :, 384:384 + RE] = gram(p3, RE)
        v['yg'][k, :, 384 + RE:] = jnp.zeros((RE, 128 - RE), F32)
        yg[0](k)

    def post_n(k):
        yn[3](k)
        p3 = stack3(v['ynT'][k])
        load_split(v['Bn'], v['sp'], k, v['Bn'].shape[1])
        v['vn'][k, :, :SN] = mm6(p3, RE, *pieces('n'), True)
        v['vn'][k, :, SN:384] = jnp.zeros((RE, 384 - SN), F32)
        v['vn'][k, :, 384:384 + RE] = gram(p3, RE)
        v['vn'][k, :, 384 + RE:] = jnp.zeros((RE, 128 - RE), F32)
        v['vnT'][k, RX:] = zero_rows

    def orth_p(l_ref, p_ref, po, k, rp):
        l3 = stack3(l_ref[k, :, :rp])
        q3 = stack3(p_ref[k])
        po[k] = mm6(l3, rp, q3[:rp], q3[rp:2 * rp], q3[2 * rp:])

    def orth_r(l_ref, y_ref, rt, k, rp, width, norm, lane):
        l3 = stack3(l_ref[k, :, :rp])
        y3 = stack3(y_ref[k, :, :width])
        res = mm6(l3, rp, y3[:rp], y3[rp:2 * rp], y3[2 * rp:])
        rt[k] = res
        col = jnp.sum(res * res, axis=1, keepdims=True)
        here = lax.broadcasted_iota(jnp.int32, (rp, 128), 1) == lane
        norm[:rp] = jnp.where(here, jnp.broadcast_to(col, (rp, 128)), norm[:rp])

    def take_d(k):
        yd[3](k)
        v['Ad'][k] = v['ydT'][k, :, SQ:]

    def take_g(k):
        yg[3](k)
        v['Ag'][k] = v['ygT'][k, :, 384:]
        v['Lg'][k, RX:] = jnp.zeros((RE - RX, 128), F32)

    def take_n(k):
        W('G', k)
        v['An'][k] = v['vnT'][k, :, 384:]
        v['Ln'][k, RX:] = jnp.zeros((RE - RX, 128), F32)

    v['st'][...] = jnp.zeros((128, 128), F32)
    v['ft'][...] = jnp.zeros((128, 128), F32)


    made, sent, copies, uses = set(), [0], [], {}

    def ship(key=None):
        made.add(key)
        while sent[0] < len(Z) and keys[sent[0]] in made:
            Z[sent[0]][0]()
            sent[0] += 1

    def last_r(k):
        W('Y', k)
        orth_r(v['Ln'], v['vnT'], v['rt_n'], k, RE, SN, v['ft'], k)

    def send_norms(_):
        v['sr'][0] = v['st'][...].T[:16]
        v['fr'][0] = v['ft'][...].T[:16]
        for d in range(1, 4):
            copies.append(remote(v['sr'].at[0], v['sr'].at[d], v['ns'].at[d], v['nr'].at[d], {'tp': lax.rem(z + d, 4)}))
            copies.append(remote(v['fr'].at[0], v['fr'].at[d], v['fs'].at[d], v['fr2'].at[d], {'fsdp': lax.rem(f + d, 4)}))
        for c in copies:
            c.start()

    table = {'S': S, 'T': T, 'Z': send_norms, 'v': last_r, 'l': post_d, 'm': post_n, 'o': post_g,
             'q': lambda k: orth_r(v['Ld'], v['ydT'], v['rt_d'], k, RD, SQ, v['st'], k),
             'r': lambda k: orth_r(v['Lg'], v['ygT'], v['rt_g'], k, RE, SN, v['st'], ND + k),
             's': lambda k: orth_p(v['Ld'], v['pdT'], v['po_d'], k, RD),
             't': lambda k: orth_p(v['Lg'], v['pgT'], v['po_g'], k, RE),
             'u': lambda k: orth_p(v['Ln'], v['ynT'], v['po_n'], k, RE)}
    for letters, steps in (('ae', yd), ('bf', yg), ('ch', yn)):
        table[letters[0]], table[letters[1]] = steps[1], steps[2]
    for letter, g in zip('ijk', 'dng'):
        table[letter] = functools.partial(part, g)
    groups = {'d': ('Ad', 'Ld', RD, RD, take_d), 'g': ('Ag', 'Lg', RX, RE, take_g), 'n': ('An', 'Ln', RX, RE, take_n)}

    def do(c):
        k = uses.get(c, 0)
        uses[c] = k + 1
        table[c](k)
        if c in 'ik':
            ship(('d' if c == 'i' else 'g', k))
        if c == 'm':
            ship(('G', k))
            ship(('Y', k))

    def do_all(todo):
        for c in todo:
            do(c)

    todo = list(SCHEDULE)
    while todo:
        c = todo.pop(0)
        if c != 'C':
            do(c)
            continue
        g, count = todo.pop(0), int(todo.pop(0))
        a, l, r, rp, take = groups[g]
        first = uses.get('C' + g, 0)
        uses['C' + g] = first + count
        duties = []
        while todo[0] != 'E':
            c = todo.pop(0)
            if c == '@':
                duties.append((ord(todo.pop(0)) - ord('A'), []))
            else:
                duties[-1][1].append(c)
        todo.pop(0)
        ks = list(range(first, first + count))
        for k in ks:
            take(k)
        chol(v[a], v[l], ks, r // 8, rp, [(at, functools.partial(do_all, d)) for at, d in duties])

    for c in copies:
        c.wait_recv()
    pad = jnp.zeros((112, 128), F32)
    tot_t = (v['sr'][0] + v['sr'][2]) + (v['sr'][1] + v['sr'][3])
    tot_f = (v['fr'][0] + v['fr'][2]) + (v['fr'][1] + v['fr'][3])
    inv_t = jnp.where(tot_t > 0.0, 1.0 / jnp.sqrt(tot_t), 0.0)
    inv_f = jnp.where(tot_f > 0.0, 1.0 / jnp.sqrt(tot_f), 0.0)
    v['inv_t'][...] = jnp.concatenate([inv_t, pad], axis=0).T
    v['inv_f'][...] = jnp.concatenate([inv_f, pad], axis=0).T

    for c in copies:
        c.wait_send()
    for piece in Z:
        piece[4]()
    for g, k in order:
        load('x', g, k).wait()
    loop(ND, yd[4])
    loop(NG, yg[4])
    loop(NE, yn[4])


def update_kernel(*refs):
    names = ['po_d', 'po_g', 'po_n', 'rt_d', 'rt_g', 'rt_n', 'inv_t', 'inv_f', 'Bd', 'Bg', 'Bn', 'Xd', 'Xg', 'Xn']
    for t in TAGS:
        names += ['X' + t, 'M' + t, 'Q' + t]
    names += ['ms', 'xs', 'qd', 'qg', 'qn', 'osem']
    v = dict(zip(names, refs))
    assert len(names) == len(refs)
    tags = [(t, None) for t in TAGS[:4]] + [(t, e) for t in TAGS[4:] for e in range(3)]

    def at(name, e):
        return v[name] if e is None else v[name].at[e]

    def slot(i):
        if i < 4:
            return 'd', i
        if i < 10:
            return 'g', i - 4
        return 'n', i - 10

    stores = []
    for i, (tag, e) in enumerate(tags):
        g, k = slot(i)
        rows = v['B' + g].shape[1]
        stores.append([pltpu.make_async_copy(v['ms'].at[i % RING, :rows], at('M' + tag, e), v['osem'].at[0, i]),
                       pltpu.make_async_copy(v['xs'].at[i % RING, :rows], at('X' + tag, e), v['osem'].at[1, i]),
                       pltpu.make_async_copy(v['q' + g].at[k], at('Q' + tag, e), v['osem'].at[2, i])])

    def pack(x):
        a, b, c = split3(x)
        return jnp.concatenate([a, b], axis=1), jnp.concatenate([a, c], axis=1)

    def packs(y):
        a, b, c = split3(y)
        return (jnp.concatenate([a, b], axis=0), jnp.concatenate([b, a], axis=0), jnp.concatenate([c, a], axis=0))

    def pad(x):
        if x.shape[0] == 128:
            return x
        return jnp.concatenate([x, jnp.zeros((128 - x.shape[0], x.shape[1]), F32)], axis=0)

    def prod(lhs, rhs):
        return dot(lhs[0], rhs[0]) + (dot(lhs[0], rhs[1]) + dot(lhs[1], rhs[2]))

    for i, (tag, e) in enumerate(tags):
        g, k = slot(i)
        pt = pad(v['po_' + g][k])
        rt = pad(v['rt_' + g][k])
        inv = v['inv_f'][:, k:k + 1] if g == 'n' else v['inv_t'][:, i:i + 1]
        qt = rt * jnp.broadcast_to(inv, rt.shape)
        flip = g != 'd'
        q = qt[:RX] if flip else qt.T
        v['q' + g][k] = q
        stores[i][2].start()
        eta = LEARN_RATE * (math.sqrt(2048 / 1408) if flip else 1.0)
        if flip:
            rhs = packs(pt)
            lhs_m, rhs_m, lhs_x, rhs_x = pack(rt.T), rhs, pack(qt.T), rhs
        else:
            lhs = pack(pt.T)
            lhs_m, rhs_m, lhs_x, rhs_x = lhs, packs(rt), lhs, packs(qt)
        rows = v['B' + g].shape[1]
        if i >= RING:
            stores[i - RING][0].wait()
            stores[i - RING][1].wait()
        v['ms'][i % RING, :rows] = v['B' + g][k] - (1.0 - MOMENTUM) * prod(lhs_m, rhs_m)
        stores[i][0].start()
        v['xs'][i % RING, :rows] = v['X' + g][k] - eta * prod(lhs_x, rhs_x)
        stores[i][1].start()
    for i, group in enumerate(stores):
        for c in group[2:] if i < len(stores) - RING else group:
            c.wait()


def vm(*shape, dtype=F32):
    return pltpu.VMEM(shape, dtype)


def solution(mesh):
    dense_w = P(('layer', 'fsdp'), 'tp')
    dense_f = P(('layer', 'tp'), None)
    stack_w = P('layer', 'fsdp', 'tp')
    stack_f = P('layer', 'tp', None)
    down_f = P('layer', 'fsdp', None)
    in_specs = (dense_w, dense_w, dense_w, dense_f) * 4 + (stack_w, stack_w, stack_w, stack_f) * 2 + (stack_w, stack_w, stack_w, down_f)
    out_specs = (dense_w, dense_w, dense_f) * 4 + (stack_w, stack_w, stack_f) * 2 + (stack_w, stack_w, down_f)
    dma = pltpu.SemaphoreType.DMA
    hbm = pl.BlockSpec(memory_space=pltpu.HBM)
    vspec = pl.BlockSpec(memory_space=pltpu.VMEM)

    def local_step(*blocks):
        mats = [blocks[4 * i:4 * i + 4] for i in range(7)]
        for i in (4, 5):
            mats[i] = tuple(jnp.swapaxes(a, 1, 2) for a in mats[i])
        mats[6] = mats[6][:3] + (jnp.swapaxes(mats[6][3], 1, 2),)
        scratch = [vm(3, SQ, SQ, dtype=BF16), vm(2, SQ, SQ, dtype=BF16), vm(SLOTS, SN, SQ, dtype=BF16), vm(ND, SQ, RD), vm(NG, RX, SN), vm(NE, RX, SN)]
        scratch += [vm(ND, RD, SQ)] * 3 + [vm(NG, RE, SQ)] * 3 + [vm(NE, RE, SQ)] * 3
        for n, rp, w in ((ND, RD, SQ + 128), (NG, RE, 512), (NE, RE, 512)):
            scratch += [vm(n, rp, w), vm(n, rp // 2, w), vm(n, rp // 2, w), vm(n, rp, w)]
        for n, rp in ((ND, RD), (NG, RE), (NE, RE)):
            scratch += [vm(n, rp, 128), vm(n, rp, 128)]
        scratch += [vm(128, 128), vm(4, 16, 128), vm(128, 128), vm(4, 16, 128)]
        scratch += [dma((4, 13))]
        scratch += [dma((3, n)) for n in (2 * ND + 1, 2 * ND + 1, 2 * NG, 2 * NG, 2 * NE, 2 * NE, ND, ND, NG, NG, NE, NE)]
        scratch += [dma((4,))] * 4
        shapes = [(ND, RD, SQ), (NG, RE, SQ), (NE, RE, SQ), (ND, RD, SQ), (NG, RE, SN), (NE, RE, SN), (128, 128), (128, 128),
                  (ND, SQ, SQ), (NG, SN, SQ), (NE, SN, SQ), (ND, SQ, SQ), (NG, SN, SQ), (NE, SN, SQ)]
        mids = pl.pallas_call(
            comm_kernel,
            out_shape=[jax.ShapeDtypeStruct(s, F32) for s in shapes],
            in_specs=[hbm] * 28,
            out_specs=[vspec] * 14,
            scratch_shapes=scratch,
            name='comm',
            compiler_params=pltpu.CompilerParams(collective_id=0, has_side_effects=True, vmem_limit_bytes=COMM_VMEM),
        )(*[pltpu.with_memory_space_constraint(a, pltpu.HBM) for m in mats for a in m])
        res = list(pl.pallas_call(
            update_kernel,
            out_shape=[jax.ShapeDtypeStruct(m[j].shape, F32) for m in mats for j in (0, 1, 3)],
            in_specs=[vspec] * 14,
            out_specs=[hbm] * 21,
            scratch_shapes=[vm(RING, SQ, SQ), vm(RING, SQ, SQ), vm(ND, SQ, RD), vm(NG, RX, SN), vm(NE, RX, SN), dma((3, 13))],
            name='update',
            compiler_params=pltpu.CompilerParams(vmem_limit_bytes=UPDATE_VMEM),
        )(*mids))
        for i in (12, 13, 14, 15, 16, 17, 20):
            res[i] = jnp.swapaxes(res[i], 1, 2)
        return tuple(res)

    return jax.shard_map(local_step, mesh=mesh, in_specs=in_specs, out_specs=out_specs, check_vma=False)
```
